32 devices in a mesh: grp: 2 (over x), sub: 16 (over z, y, core).
Axes of the slice: x: 2, y: 2, z: 4, core: 2. Of those that a mesh axis runs over, the one named last changes fastest.
Arguments:
- counts: int32 [32], P(('grp', 'sub')), may hold values from 1 to 3, as said below
- block_map: int32 [96], P(('grp', 'sub')), may hold values from 0 to 31
- perms: int32 [96, 256], P(('grp', 'sub')), may hold values from 0 to 255, each once within a row
- mass_ii: bfloat16 [96, 1024, 1024], P(('grp', 'sub')), may hold values from -0.005859375 to 0.005859375
- mass_ib: bfloat16 [96, 1024, 256], P(('grp', 'sub')), may hold values from -0.1875 to 0.1875
- mass_bb: bfloat16 [96, 256, 256], P(('grp', 'sub')), may hold values from -6 to 6
- constraint_modes: bfloat16 [96, 1024, 256], P(('grp', 'sub')), may hold values from -6 to 6
- fixed_modes: bfloat16 [96, 1024, 128], P(('grp', 'sub')), may hold values from -6 to 6
Outputs:
- blocks: float32 [32, 256, 256], P('grp', 'sub')
- coupling: float32 [96, 128, 256], P(('grp', 'sub'))
The draws below stay inside these ranges and needn't reach their ends.
Inputs may be any that keep to these rules, and one draw needn't show every extreme that they name: `counts`: at least one device uses all 3 slots and one uses a single slot.
All inputs are finite; a program needn't handle non-finite values.
Results may differ from the reference program's by a relative error of at most 0.0021.
Values sent between devices are 32-bit elements; how exact they have to be, the bound alone decides.
A program may use at most 128 MiB of HBM per device.

```python
import jax
import jax.numpy as jnp
from jax import lax

I = 1024
B = 256
K = 128
SLOTS = 3
NBG = 16
CAP = 96
N_GRP = 2
N_SUB = 16
DEVICES = 32


def draw_counts(key, part):
    raw = jax.random.randint(key, (DEVICES,), 0, 6)
    values = jnp.where(raw < 4, 1, jnp.where(raw == 4, 2, SLOTS))
    values = jnp.minimum(values, SLOTS)
    values = values.at[0].set(SLOTS).at[1].set(1)
    return values.astype(jnp.int32)


def place_ends(drawn, own_key, low, high):
    extent = drawn.shape
    place = [jax.random.randint(jax.random.fold_in(own_key, axis), (), 0, extent[axis]) for axis in range(len(extent))]
    drawn = drawn.at[tuple(place)].set(low)
    longest = extent.index(max(extent))
    place[longest] = (place[longest] + 1) % extent[longest]
    return drawn.at[tuple(place)].set(high)


def shard_levels(stream_key, shape, cuts, low, high):
    level, own = 1.0, jax.random.fold_in(stream_key, 6)
    for axis_at, parts in cuts:
        heights = jnp.exp(jax.random.uniform(jax.random.fold_in(own, axis_at), (parts,), jnp.float32, low / len(cuts), high / len(cuts)))
        level = level * jnp.repeat(heights, shape[axis_at] // parts).reshape([-1 if axis == axis_at else 1 for axis in range(len(shape))])
    return level


def scatter_about(key, extent, deviation, bound, shards=(), held_as=jnp.bfloat16):
    drawn = jax.random.normal(key, extent, jnp.float32) * deviation
    if len(shards) > 0:
        drawn = shard_levels(key, extent, shards, -0.22, 0.18) * drawn
    return jnp.clip(drawn, min=-bound, max=bound).astype(held_as)


def setup_inputs(seed: int = 0) -> dict:
    keys = jax.random.split(jax.random.key(seed), 9)
    return {
        "counts": draw_counts(jax.random.fold_in(keys[8], 71), 0),
        "block_map": place_ends(jax.random.randint(keys[1], (CAP,), 0, 2 * NBG), jax.random.fold_in(keys[1], 1), 0, (2 * NBG) - 1).astype(jnp.int32),
        "perms": jax.vmap(lambda own: jax.random.permutation(own, B))(jax.random.split(keys[2], CAP)).reshape((CAP, B)).astype(jnp.int32),
        "mass_ii": scatter_about(keys[3], (CAP, I, I), (I * I) ** -0.5, 0.005859375, ((0, 32),)),
        "mass_ib": scatter_about(keys[4], (CAP, I, B), I ** -0.5, 0.1875, ((0, 32),)),
        "mass_bb": scatter_about(keys[5], (CAP, B, B), 1.0, 6.0, ((0, 32),)),
        "constraint_modes": scatter_about(keys[6], (CAP, I, B), 1.0, 6.0, ((0, 32),)),
        "fixed_modes": scatter_about(keys[7], (CAP, I, K), 1.0, 6.0, ((0, 32),)),
    }


def contract(left, right):
    return lax.dot_general(left, right, (((0,), (0,)), ((), ())), preferred_element_type=jnp.float32)


def reduce_slot(mass_ii, mass_ib, mass_bb, constraint_modes, fixed_modes):
    product = jnp.dot(mass_ii, constraint_modes, preferred_element_type=jnp.float32).astype(jnp.bfloat16)
    cross = contract(constraint_modes, mass_ib)
    reduced = contract(constraint_modes, product) + cross + cross.T + mass_bb.astype(jnp.float32)
    coupled = contract(fixed_modes, product) + contract(fixed_modes, mass_ib)
    return reduced, coupled


def reference(counts, block_map, perms, mass_ii, mass_ib, mass_bb, constraint_modes, fixed_modes):
    width = mass_bb.shape[1]
    total_slots = mass_ii.shape[0]
    modes = fixed_modes.shape[2]

    def step(carry_blocks, items):
        slot_id, code, perm_row, m_ii, m_ib, m_bb, psi_slot, phi_slot = items
        device = slot_id // SLOTS
        used_flag = (slot_id % SLOTS) < counts[device]
        group_index = device // N_SUB

        def active_branch(unused):
            return reduce_slot(m_ii, m_ib, m_bb, psi_slot, phi_slot)

        def empty_branch(unused):
            return (jnp.zeros((width, width), jnp.float32), jnp.zeros((modes, width), jnp.float32))

        reduced, coupled = lax.cond(used_flag, active_branch, empty_branch, 0)
        target = ((group_index + code // NBG) % N_GRP) * NBG + code % NBG
        inverse = jnp.zeros((width,), jnp.int32).at[perm_row].set(jnp.arange(width, dtype=jnp.int32))
        placed = reduced[inverse][:, inverse]
        carry_blocks = carry_blocks.at[target.astype(jnp.int32)].add(placed)
        return carry_blocks, coupled

    start = jnp.zeros((NBG * N_GRP, width, width), jnp.float32)
    items = (jnp.arange(total_slots, dtype=jnp.int32), block_map, perms, mass_ii, mass_ib, mass_bb, constraint_modes, fixed_modes)
    blocks, coupling = lax.scan(step, start, items)
    return blocks, coupling
```

```python
import functools

import jax
import jax.numpy as jnp
from jax import lax
from jax.experimental import pallas as pl
from jax.experimental.pallas import tpu as pltpu
from jax.sharding import PartitionSpec as P

NBG = 16
ROWS = 8
LANES = 128
WINDOW = 2
STRIPS = 4
MESH = pl.DeviceIdType.MESH


def split(value):
    high = value.astype(jnp.bfloat16)
    low = (value - high.astype(jnp.float32)).astype(jnp.bfloat16)
    return high, low


def dot(left, right, left_dim=1, right_dim=0):
    return lax.dot_general(
        left,
        right,
        (((left_dim,), (right_dim,)), ((), ())),
        preferred_element_type=jnp.float32,
    )


def send_order(peers):
    return sorted(range(1, peers), key=lambda step: (abs(step - peers // 2), step))


def kernel(
    n_grp,
    n_sub,
    counts,
    codes,
    perms,
    mass_ii,
    mass_ib,
    mass_bb,
    psi_in,
    phi_in,
    blocks,
    coupling,
    m_ii,
    m_bb,
    lhs,
    rhs,
    placed,
    got,
    key_mine,
    key_got,
    hot,
    sums,
    passed,
    in_sem,
    send_sem,
    got_sem,
    key_send_sem,
    key_sem,
    pass_send_sem,
    pass_sem,
):
    grp = lax.axis_index("grp")
    me = lax.axis_index("sub")
    slots, interior, width = psi_in.shape
    chunks = got.shape[0]
    cuts = width // LANES
    own_rows = chunks // cuts * ROWS
    lanes = n_sub * ROWS
    after = lax.rem(grp + 1, n_grp)
    before = lax.rem(grp + n_grp - 1, n_grp)

    def loads(slot):
        pairs = (
            (psi_in, lhs.at[slot, :, pl.ds(0, width)]),
            (mass_ii, m_ii.at[slot]),
            (mass_ib, rhs.at[slot, :, pl.ds(width, width)]),
            (mass_bb, m_bb.at[slot]),
            (phi_in, lhs.at[slot, :, pl.ds(width, lhs.shape[2] - width)]),
        )
        return [
            pltpu.make_async_copy(source.at[slot], held, in_sem.at[slot, index])
            for index, (source, held) in enumerate(pairs)
        ]

    for copy in loads(0):
        copy.start()

    order = send_order(n_sub)
    peers = [lax.rem(me + step, n_sub) for step in order]
    barrier = pltpu.get_barrier_semaphore()
    for peer in peers:
        pl.semaphore_signal(barrier, inc=1, device_id=(grp, peer), device_id_type=MESH)
    pl.semaphore_signal(barrier, inc=1, device_id=(after, me), device_id_type=MESH)
    greeted = len(peers) + 1
    if n_grp > 2:
        pl.semaphore_signal(barrier, inc=1, device_id=(before, me), device_id_type=MESH)
        greeted += 1

    lane = lax.broadcasted_iota(jnp.int32, (1, lanes), 1)
    key_mine[...] = jnp.zeros_like(key_mine)
    for slot in range(slots):
        code = jnp.where(slot < counts[0], codes[slot] * ROWS, -2 * NBG * ROWS)
        key_mine[slot : slot + 1, :] = jnp.where(lane // ROWS == me, code + lane % ROWS, 0)
    key_got[pl.ds(me, 1)] = key_mine[...][None]

    def key_copy(peer):
        return pltpu.make_async_remote_copy(
            src_ref=key_mine,
            dst_ref=key_got.at[me],
            send_sem=key_send_sem,
            recv_sem=key_sem,
            device_id=(grp, peer),
            device_id_type=MESH,
        )

    def send(chunk, slot):
        for peer in peers:
            top = pl.multiple_of(peer * own_rows + chunk // cuts * ROWS, ROWS)
            left = chunk % cuts * LANES
            pltpu.make_async_remote_copy(
                src_ref=placed.at[slot, pl.ds(top, ROWS), pl.ds(left, LANES)],
                dst_ref=got.at[chunk, slot, me],
                send_sem=send_sem.at[chunk, slot],
                recv_sem=got_sem.at[chunk, slot],
                device_id=(grp, peer),
                device_id_type=MESH,
            ).start()

    @pl.loop(0, slots)
    def one_slot(slot):
        copies = loads(slot)

        @pl.when(slot + 1 < slots)
        def ahead_loads():
            for copy in loads(slot + 1):
                copy.start()

        copies[0].wait()
        copies[1].wait()
        step = min(interior, 256)
        modes = lhs[slot, :, :width]
        for top in range(0, interior, step):
            made = dot(m_ii[slot, top : top + step, :], modes).astype(jnp.bfloat16)
            rhs[slot, top : top + step, :width] = made
        for copy in copies[2:]:
            copy.wait()
        every = dot(lhs[slot], rhs[slot], 0, 0)
        cross = every[:width, width:]
        direct = every[:width, :width] + cross + m_bb[slot].astype(jnp.float32)
        place = lax.broadcasted_iota(jnp.int32, (width, width), 0)
        pick = jnp.where(place == perms[pl.ds(slot, 1), :], 1.0, 0.0).astype(jnp.bfloat16)
        high, low = split(direct)
        cross_high, cross_low = split(cross)
        rows = dot(pick, high) + dot(pick, low)
        rows = rows + dot(pick, cross_high, 1, 1) + dot(pick, cross_low, 1, 1)
        high, low = split(rows)
        placed[slot] = dot(high, pick, 1, 1) + dot(low, pick, 1, 1)
        active = jnp.where(slot < counts[0], 1.0, 0.0)
        coupling[slot] = (every[width:, :width] + every[width:, width:]) * active
        for chunk in range(chunks):
            mine = pl.multiple_of(me * own_rows + chunk // cuts * ROWS, ROWS)
            left = chunk % cuts * LANES
            own = placed[slot, pl.ds(mine, ROWS), left : left + LANES]
            got[chunk, slot, pl.ds(me, 1)] = own[None]

        @pl.when(slot == 0)
        def enter():
            pl.semaphore_wait(barrier, greeted)
            for peer in peers:
                key_copy(peer).start()

        @pl.when(slot < slots - 1)
        def spread():
            for chunk in range(chunks):
                send(chunk, slot)

    window = min(WINDOW, chunks)
    for chunk in range(window):
        send(chunk, slots - 1)

    many = n_sub - 1
    all_keys = key_got.at[pl.ds(0, many)]
    pltpu.make_async_copy(all_keys, all_keys, key_sem).wait()
    keys = jnp.sum(key_got[...], axis=0)
    target = lax.broadcasted_iota(jnp.int32, (2 * NBG * ROWS, lanes), 0)
    for slot in range(slots):
        hot[slot] = jnp.where(target == keys[slot : slot + 1, :], 1.0, 0.0).astype(jnp.bfloat16)

    def pass_copy(chunk):
        return pltpu.make_async_remote_copy(
            src_ref=sums.at[chunk, pl.ds(NBG * ROWS, NBG * ROWS)],
            dst_ref=passed.at[chunk],
            send_sem=pass_send_sem.at[chunk],
            recv_sem=pass_sem.at[chunk],
            device_id=(after, me),
            device_id_type=MESH,
        )

    def owner_sum(chunk, slot):
        arrived = got.at[chunk, slot, pl.ds(0, many)]
        pltpu.make_async_copy(arrived, arrived, got_sem.at[chunk, slot]).wait()
        high, low = split(got[chunk, slot].reshape(lanes, LANES))
        return dot(hot[slot], high) + dot(hot[slot], low)

    for slot in range(slots):
        for chunk in range(chunks):
            total = owner_sum(chunk, slot)
            if slot > 0:
                total = total + sums[chunk]
            sums[chunk] = total
            if slot == slots - 1:
                pass_copy(chunk).start()
                if chunk + window < chunks:
                    send(chunk + window, slot)

    for chunk in range(chunks):
        pass_copy(chunk).wait()
        own = sums[chunk, : NBG * ROWS] + passed[chunk]
        top, left = chunk // cuts * ROWS, chunk % cuts * LANES
        blocks[:, top : top + ROWS, left : left + LANES] = own.reshape(NBG, ROWS, LANES)

    pltpu.make_async_copy(all_keys, all_keys, key_send_sem).wait()
    for chunk in range(chunks):
        for slot in range(slots):
            arrived = got.at[chunk, slot, pl.ds(0, many)]
            pltpu.make_async_copy(arrived, arrived, send_sem.at[chunk, slot]).wait()


def cross_kernel(
    n_grp,
    n_sub,
    counts,
    codes,
    perms,
    mass_ii,
    mass_ib,
    mass_bb,
    psi_in,
    phi_in,
    blocks,
    coupling,
    m_ii,
    m_bb,
    lhs,
    rhs,
    placed,
    near,
    far,
    held,
    key_mine,
    key_got,
    hot,
    sums,
    part,
    passed,
    landed,
    in_sem,
    send_sem,
    got_sem,
    key_send_sem,
    key_sem,
    pass_send_sem,
    pass_sem,
):
    grp = lax.axis_index("grp")
    me = lax.axis_index("sub")
    slots, interior, width = psi_in.shape
    own_rows = width // n_sub
    half = n_sub // 2
    lanes = n_sub * ROWS
    part_rows = NBG * ROWS
    cut = width // 2
    quad = half // 2
    other = 1 - grp
    spot = lax.rem(me, half)
    first = me - spot
    beyond = half - first
    twin = beyond + spot
    member = grp * half + spot
    reach = grp + me // quad + lax.rem(me // 2, 2)
    gate = jnp.maximum(slots - 1 - reach, 0)

    def loads(slot):
        pairs = (
            (psi_in, lhs.at[slot, :, pl.ds(0, width)]),
            (mass_ii, m_ii.at[slot]),
            (mass_ib, rhs.at[slot, :, pl.ds(width, width)]),
            (mass_bb, m_bb.at[slot]),
            (phi_in, lhs.at[slot, :, pl.ds(width, lhs.shape[2] - width)]),
        )
        return [
            pltpu.make_async_copy(source.at[slot], into, in_sem.at[slot, index])
            for index, (source, into) in enumerate(pairs)
        ]

    for slot in range(slots):
        for copy in loads(slot):
            copy.start()

    def peer_at(base, plane, turn, step):
        low = plane * quad + lax.rem(me + step, quad)
        return lax.rem(grp + turn, n_grp), base + low

    steps = [(1, 2), (0, 2), (1, 3), (0, 3), (1, 1), (1, 0), (0, 1), (0, 0)]
    across = [peer_at(beyond, plane, *step) for plane in range(2) for step in steps]
    close = [
        (peer_at(first, plane, *step), None if step != (0, 0) else spot // quad != plane)
        for plane in range(2)
        for step in steps
    ]
    barrier = pltpu.get_barrier_semaphore()

    def greet(peer):
        pl.semaphore_signal(barrier, inc=1, device_id=peer, device_id_type=MESH)

    def each_close(act):
        for peer, other_one in close:
            if other_one is None:
                act(peer)
            else:
                pl.when(other_one)(functools.partial(act, peer))

    for peer in across:
        greet(peer)
    each_close(greet)

    lane = lax.broadcasted_iota(jnp.int32, (1, lanes), 1)
    for slot in range(slots):
        code = codes[slot]
        block = lax.rem(grp + code // NBG, n_grp) * NBG + lax.rem(code, NBG)
        block = jnp.where(slot < counts[0], block, -n_grp * NBG) * ROWS
        key_mine[slot] = jnp.where(lane // ROWS == member, block + lane % ROWS, 0)
    key_got[0, pl.ds(member, 1)] = key_mine[...][None]

    def row_of(peer, owner):
        return pl.multiple_of(owner * own_rows + peer[0] * ROWS, ROWS)

    def push(source, into, kind, slot, peer):
        pltpu.make_async_remote_copy(
            src_ref=source,
            dst_ref=into,
            send_sem=send_sem.at[kind, slot],
            recv_sem=got_sem.at[kind, slot],
            device_id=peer,
            device_id_type=MESH,
        ).start()

    def send_keys():
        def key_copy(side, peer):
            pltpu.make_async_remote_copy(
                src_ref=key_mine,
                dst_ref=key_got.at[side, member],
                send_sem=key_send_sem.at[side],
                recv_sem=key_sem.at[side],
                device_id=peer,
                device_id_type=MESH,
            ).start()

        for peer in across:
            key_copy(1, peer)
        each_close(functools.partial(key_copy, 0))

    def send_far(slot):
        for peer in across:
            rows = pl.ds(row_of(peer, peer[1]), ROWS)
            push(placed.at[slot, rows, pl.ds(0, cut)], far.at[slot, member], 0, slot, peer)

    def held_rows(peer):
        return pl.ds(row_of(peer, beyond + peer[1] - first), ROWS)

    def send_held(slot):
        def one(peer):
            source = placed.at[slot, held_rows(peer), pl.ds(cut, cut)]
            push(source, held.at[slot, member], 1, slot, peer)

        each_close(one)

    def send_near(slot):
        def one(peer):
            rows = pl.ds(row_of(peer, peer[1]), ROWS)
            push(placed.at[slot, rows, :], near.at[slot, member], 2, slot, peer)

        each_close(one)

    def spread(slot):
        send_far(slot)
        send_held(slot)
        if slot > 0:
            send_near(slot - 1)

    def reduce_slot(slot):
        for copy in loads(slot):
            copy.wait()
        modes = lhs[slot, :, :width]
        step = interior // STRIPS
        for top in range(0, interior, step):
            made = dot(m_ii[slot, top : top + step, :], modes).astype(jnp.bfloat16)
            rhs[slot, top : top + step, :width] = made
        every = dot(lhs[slot], rhs[slot], 0, 0)
        cross = every[:width, width:]
        direct = every[:width, :width] + cross + m_bb[slot].astype(jnp.float32)
        place = lax.broadcasted_iota(jnp.int32, (width, width), 0)
        pick = jnp.where(place == perms[pl.ds(slot, 1), :], 1.0, 0.0).astype(jnp.bfloat16)
        high, low = split(direct)
        cross_high, cross_low = split(cross)
        rows = dot(pick, high) + dot(pick, low)
        rows = rows + dot(pick, cross_high, 1, 1) + dot(pick, cross_low, 1, 1)
        high, low = split(rows)
        placed[slot] = dot(high, pick, 1, 1) + dot(low, pick, 1, 1)
        active = jnp.where(slot < counts[0], 1.0, 0.0)
        coupling[slot] = (every[width:, :width] + every[width:, width:]) * active
        mine = pl.ds(row_of((grp, me), me), ROWS)
        near[slot, pl.ds(member, 1)] = placed[slot, mine, :][None]
        mine = pl.ds(row_of((grp, me), twin), ROWS)
        held[slot, pl.ds(member, 1)] = placed[slot, mine, pl.ds(cut, cut)][None]

    for slot in range(slots):
        reduce_slot(slot)

        @pl.when(gate == slot)
        def enter():
            pl.semaphore_wait(barrier, 2 * n_sub - 1)
            send_keys()
            for early in range(slot):
                spread(early)

        @pl.when(gate <= slot)
        def follow():
            spread(slot)

    send_near(slots - 1)

    many = n_sub - 1

    def settle(ref, sem):
        pltpu.make_async_copy(ref, ref, sem).wait()

    settle(key_got.at[0, pl.ds(0, many)], key_sem.at[0])
    settle(key_got.at[1], key_sem.at[1])
    target = lax.broadcasted_iota(jnp.int32, (n_grp * part_rows, lanes), 0)
    for side in range(2):
        keys = jnp.sum(key_got[side], axis=0)
        for slot in range(slots):
            hot[side, slot] = jnp.where(target == keys[slot], 1.0, 0.0).astype(jnp.bfloat16)

    def gather(side, slot, got):
        high, low = split(got.reshape(lanes, got.shape[-1]))
        return dot(hot[side, slot], high) + dot(hot[side, slot], low)

    total = None
    for slot in range(slots):
        settle(held.at[slot, pl.ds(0, many)], got_sem.at[1, slot])
        one = gather(0, slot, held[slot])
        total = one if total is None else total + one
    part[...] = total

    def hand(to):
        return pltpu.make_async_remote_copy(
            src_ref=part.at[pl.ds(pl.multiple_of(to * part_rows, part_rows), part_rows)],
            dst_ref=landed.at[grp],
            send_sem=pass_send_sem.at[0],
            recv_sem=pass_sem.at[grp],
            device_id=(to, twin),
            device_id_type=MESH,
        )

    hand(other).start()
    hand(grp).start()

    total = None
    for slot in range(slots):
        settle(near.at[slot, pl.ds(0, many)], got_sem.at[2, slot])
        one = gather(0, slot, near[slot])
        total = one if total is None else total + one
    sums[...] = total
    total = None
    for slot in range(slots):
        settle(far.at[slot], got_sem.at[0, slot])
        one = gather(1, slot, far[slot])
        total = one if total is None else total + one
    sums[:, :cut] = sums[:, :cut] + total
    swap = pltpu.make_async_remote_copy(
        src_ref=sums.at[pl.ds(pl.multiple_of(other * part_rows, part_rows), part_rows)],
        dst_ref=passed,
        send_sem=pass_send_sem.at[1],
        recv_sem=pass_sem.at[2],
        device_id=(other, me),
        device_id_type=MESH,
    )
    swap.start()

    settle(key_got.at[0, pl.ds(0, many)], key_send_sem.at[0])
    settle(key_got.at[1], key_send_sem.at[1])
    for slot in range(slots):
        settle(far.at[slot], send_sem.at[0, slot])
        settle(held.at[slot, pl.ds(0, many)], send_sem.at[1, slot])
        settle(near.at[slot, pl.ds(0, many)], send_sem.at[2, slot])

    kept = sums[pl.ds(pl.multiple_of(grp * part_rows, part_rows), part_rows), :]
    swap.wait()
    for row, value in ((grp, kept), (other, passed[...])):
        into = pl.ds(pl.multiple_of(row * ROWS, ROWS), ROWS)
        blocks[:, into, :cut] = value[:, :cut].reshape(NBG, ROWS, cut)
    settle(landed.at[0], pass_sem.at[0])
    settle(landed.at[1], pass_sem.at[1])
    for row, value in ((grp, kept), (other, passed[...])):
        into = pl.ds(pl.multiple_of(row * ROWS, ROWS), ROWS)
        late = value[:, cut:] + landed[row]
        blocks[:, into, cut:] = late.reshape(NBG, ROWS, cut)
    settle(landed, pass_send_sem.at[0])


def cross_scratch(n_grp, n_sub, slots, interior, width, modes):
    bf16, f32, i32 = jnp.bfloat16, jnp.float32, jnp.int32
    dma = pltpu.SemaphoreType.DMA
    lanes, cut = n_sub * ROWS, width // 2
    total = n_grp * NBG * ROWS
    return [
        pltpu.VMEM((slots, interior, interior), bf16),
        pltpu.VMEM((slots, width, width), bf16),
        pltpu.VMEM((slots, interior, width + modes), bf16),
        pltpu.VMEM((slots, interior, 2 * width), bf16),
        pltpu.VMEM((slots, width, width), f32),
        pltpu.VMEM((slots, n_sub, ROWS, width), f32),
        pltpu.VMEM((slots, n_sub, ROWS, cut), f32),
        pltpu.VMEM((slots, n_sub, ROWS, cut), f32),
        pltpu.VMEM((slots, 1, lanes), i32),
        pltpu.VMEM((2, n_sub, slots, 1, lanes), i32),
        pltpu.VMEM((2, slots, total, lanes), bf16),
        pltpu.VMEM((total, width), f32),
        pltpu.VMEM((total, cut), f32),
        pltpu.VMEM((NBG * ROWS, width), f32),
        pltpu.VMEM((n_grp, NBG * ROWS, cut), f32),
        dma((slots, 5)),
        dma((3, slots)),
        dma((3, slots)),
        dma((2,)),
        dma((2,)),
        dma((2,)),
        dma((3,)),
    ]


def per_device(n_grp, n_sub, counts, block_map, perms, mass_ii, mass_ib, mass_bb, psi, phi):
    slots, interior, width = psi.shape
    modes = phi.shape[2]
    own_rows = width // n_sub
    chunks = own_rows // ROWS * (width // LANES)
    lanes = n_sub * ROWS
    body = kernel
    fits = n_grp == 2 and n_sub * ROWS == LANES and own_rows == 2 * ROWS and width == 2 * LANES
    key_rows = -(-slots // 8) * 8
    smem = pl.BlockSpec(memory_space=pltpu.SMEM)
    vmem = pl.BlockSpec(memory_space=pltpu.VMEM)
    hbm = pl.BlockSpec(memory_space=pl.ANY)
    bf16, f32, i32 = jnp.bfloat16, jnp.float32, jnp.int32
    dma = pltpu.SemaphoreType.DMA
    scratch = [
        pltpu.VMEM(mass_ii.shape, bf16),
        pltpu.VMEM(mass_bb.shape, bf16),
        pltpu.VMEM((slots, interior, width + modes), bf16),
        pltpu.VMEM((slots, interior, 2 * width), bf16),
        pltpu.VMEM((slots, width, width), f32),
        pltpu.VMEM((chunks, slots, n_sub, ROWS, LANES), f32),
        pltpu.VMEM((key_rows, lanes), i32),
        pltpu.VMEM((n_sub, key_rows, lanes), i32),
        pltpu.VMEM((slots, 2 * NBG * ROWS, lanes), bf16),
        pltpu.VMEM((chunks, 2 * NBG * ROWS, LANES), f32),
        pltpu.VMEM((chunks, NBG * ROWS, LANES), f32),
        dma((slots, 5)),
        dma((chunks, slots)),
        dma((chunks, slots)),
        dma,
        dma,
        dma((chunks,)),
        dma((chunks,)),
    ]
    if fits and interior % STRIPS == 0:
        body = cross_kernel
        scratch = cross_scratch(n_grp, n_sub, slots, interior, width, modes)
    return pl.pallas_call(
        functools.partial(body, n_grp, n_sub),
        out_shape=(
            pltpu.VMEM((NBG, own_rows, width), f32),
            pltpu.VMEM((slots, modes, width), f32),
        ),
        in_specs=[smem, smem, vmem] + [hbm] * 5,
        out_specs=(vmem, vmem),
        scratch_shapes=scratch,
        compiler_params=pltpu.CompilerParams(
            collective_id=0, has_side_effects=True, vmem_limit_bytes=56 * 1024 * 1024
        ),
    )(counts, block_map, perms, mass_ii, mass_ib, mass_bb, psi, phi)


def solution(mesh):
    both = P(("grp", "sub"))
    return jax.shard_map(
        functools.partial(per_device, mesh.shape["grp"], mesh.shape["sub"]),
        mesh=mesh,
        in_specs=(both,) * 8,
        out_specs=(P("grp", "sub", None), both),
        check_vma=False,
    )
```

```python
import functools

import jax
import jax.numpy as jnp
from jax import lax
from jax.experimental import pallas as pl
from jax.experimental.pallas import tpu as pltpu
from jax.sharding import PartitionSpec as P

NBG = 16
ROWS = 8
LANES = 128
WINDOW = 2
STRIPS = 4
MESH = pl.DeviceIdType.MESH


def split(value):
    high = value.astype(jnp.bfloat16)
    low = (value - high.astype(jnp.float32)).astype(jnp.bfloat16)
    return high, low


def dot(left, right, left_dim=1, right_dim=0):
    return lax.dot_general(
        left,
        right,
        (((left_dim,), (right_dim,)), ((), ())),
        preferred_element_type=jnp.float32,
    )


def send_order(peers):
    return sorted(range(1, peers), key=lambda step: (abs(step - peers // 2), step))


def kernel(
    n_grp,
    n_sub,
    counts,
    codes,
    perms,
    mass_ii,
    mass_ib,
    mass_bb,
    psi_in,
    phi_in,
    blocks,
    coupling,
    m_ii,
    m_bb,
    lhs,
    rhs,
    placed,
    got,
    key_mine,
    key_got,
    hot,
    sums,
    passed,
    in_sem,
    send_sem,
    got_sem,
    key_send_sem,
    key_sem,
    pass_send_sem,
    pass_sem,
):
    grp = lax.axis_index("grp")
    me = lax.axis_index("sub")
    slots, interior, width = psi_in.shape
    chunks = got.shape[0]
    cuts = width // LANES
    own_rows = chunks // cuts * ROWS
    lanes = n_sub * ROWS
    after = lax.rem(grp + 1, n_grp)
    before = lax.rem(grp + n_grp - 1, n_grp)

    def loads(slot):
        pairs = (
            (psi_in, lhs.at[slot, :, pl.ds(0, width)]),
            (mass_ii, m_ii.at[slot]),
            (mass_ib, rhs.at[slot, :, pl.ds(width, width)]),
            (mass_bb, m_bb.at[slot]),
            (phi_in, lhs.at[slot, :, pl.ds(width, lhs.shape[2] - width)]),
        )
        return [
            pltpu.make_async_copy(source.at[slot], held, in_sem.at[slot, index])
            for index, (source, held) in enumerate(pairs)
        ]

    for copy in loads(0):
        copy.start()

    order = send_order(n_sub)
    peers = [lax.rem(me + step, n_sub) for step in order]
    barrier = pltpu.get_barrier_semaphore()
    for peer in peers:
        pl.semaphore_signal(barrier, inc=1, device_id=(grp, peer), device_id_type=MESH)
    pl.semaphore_signal(barrier, inc=1, device_id=(after, me), device_id_type=MESH)
    greeted = len(peers) + 1
    if n_grp > 2:
        pl.semaphore_signal(barrier, inc=1, device_id=(before, me), device_id_type=MESH)
        greeted += 1

    lane = lax.broadcasted_iota(jnp.int32, (1, lanes), 1)
    key_mine[...] = jnp.zeros_like(key_mine)
    for slot in range(slots):
        code = jnp.where(slot < counts[0], codes[slot] * ROWS, -2 * NBG * ROWS)
        key_mine[slot : slot + 1, :] = jnp.where(lane // ROWS == me, code + lane % ROWS, 0)
    key_got[pl.ds(me, 1)] = key_mine[...][None]

    def key_copy(peer):
        return pltpu.make_async_remote_copy(
            src_ref=key_mine,
            dst_ref=key_got.at[me],
            send_sem=key_send_sem,
            recv_sem=key_sem,
            device_id=(grp, peer),
            device_id_type=MESH,
        )

    def send(chunk, slot):
        for peer in peers:
            top = pl.multiple_of(peer * own_rows + chunk // cuts * ROWS, ROWS)
            left = chunk % cuts * LANES
            pltpu.make_async_remote_copy(
                src_ref=placed.at[slot, pl.ds(top, ROWS), pl.ds(left, LANES)],
                dst_ref=got.at[chunk, slot, me],
                send_sem=send_sem.at[chunk, slot],
                recv_sem=got_sem.at[chunk, slot],
                device_id=(grp, peer),
                device_id_type=MESH,
            ).start()

    @pl.loop(0, slots)
    def one_slot(slot):
        copies = loads(slot)

        @pl.when(slot + 1 < slots)
        def ahead_loads():
            for copy in loads(slot + 1):
                copy.start()

        copies[0].wait()
        copies[1].wait()
        step = min(interior, 256)
        modes = lhs[slot, :, :width]
        for top in range(0, interior, step):
            made = dot(m_ii[slot, top : top + step, :], modes).astype(jnp.bfloat16)
            rhs[slot, top : top + step, :width] = made
        for copy in copies[2:]:
            copy.wait()
        every = dot(lhs[slot], rhs[slot], 0, 0)
        cross = every[:width, width:]
        direct = every[:width, :width] + cross + m_bb[slot].astype(jnp.float32)
        place = lax.broadcasted_iota(jnp.int32, (width, width), 0)
        pick = jnp.where(place == perms[pl.ds(slot, 1), :], 1.0, 0.0).astype(jnp.bfloat16)
        high, low = split(direct)
        cross_high, cross_low = split(cross)
        rows = dot(pick, high) + dot(pick, low)
        rows = rows + dot(pick, cross_high, 1, 1) + dot(pick, cross_low, 1, 1)
        high, low = split(rows)
        placed[slot] = dot(high, pick, 1, 1) + dot(low, pick, 1, 1)
        active = jnp.where(slot < counts[0], 1.0, 0.0)
        coupling[slot] = (every[width:, :width] + every[width:, width:]) * active
        for chunk in range(chunks):
            mine = pl.multiple_of(me * own_rows + chunk // cuts * ROWS, ROWS)
            left = chunk % cuts * LANES
            own = placed[slot, pl.ds(mine, ROWS), left : left + LANES]
            got[chunk, slot, pl.ds(me, 1)] = own[None]

        @pl.when(slot == 0)
        def enter():
            pl.semaphore_wait(barrier, greeted)
            for peer in peers:
                key_copy(peer).start()

        @pl.when(slot < slots - 1)
        def spread():
            for chunk in range(chunks):
                send(chunk, slot)

    window = min(WINDOW, chunks)
    for chunk in range(window):
        send(chunk, slots - 1)

    many = n_sub - 1
    all_keys = key_got.at[pl.ds(0, many)]
    pltpu.make_async_copy(all_keys, all_keys, key_sem).wait()
    keys = jnp.sum(key_got[...], axis=0)
    target = lax.broadcasted_iota(jnp.int32, (2 * NBG * ROWS, lanes), 0)
    for slot in range(slots):
        hot[slot] = jnp.where(target == keys[slot : slot + 1, :], 1.0, 0.0).astype(jnp.bfloat16)

    def pass_copy(chunk):
        return pltpu.make_async_remote_copy(
            src_ref=sums.at[chunk, pl.ds(NBG * ROWS, NBG * ROWS)],
            dst_ref=passed.at[chunk],
            send_sem=pass_send_sem.at[chunk],
            recv_sem=pass_sem.at[chunk],
            device_id=(after, me),
            device_id_type=MESH,
        )

    def owner_sum(chunk, slot):
        arrived = got.at[chunk, slot, pl.ds(0, many)]
        pltpu.make_async_copy(arrived, arrived, got_sem.at[chunk, slot]).wait()
        high, low = split(got[chunk, slot].reshape(lanes, LANES))
        return dot(hot[slot], high) + dot(hot[slot], low)

    for slot in range(slots):
        for chunk in range(chunks):
            total = owner_sum(chunk, slot)
            if slot > 0:
                total = total + sums[chunk]
            sums[chunk] = total
            if slot == slots - 1:
                pass_copy(chunk).start()
                if chunk + window < chunks:
                    send(chunk + window, slot)

    for chunk in range(chunks):
        pass_copy(chunk).wait()
        own = sums[chunk, : NBG * ROWS] + passed[chunk]
        top, left = chunk // cuts * ROWS, chunk % cuts * LANES
        blocks[:, top : top + ROWS, left : left + LANES] = own.reshape(NBG, ROWS, LANES)

    pltpu.make_async_copy(all_keys, all_keys, key_send_sem).wait()
    for chunk in range(chunks):
        for slot in range(slots):
            arrived = got.at[chunk, slot, pl.ds(0, many)]
            pltpu.make_async_copy(arrived, arrived, send_sem.at[chunk, slot]).wait()


def cross_kernel(
    n_grp,
    n_sub,
    counts_in,
    codes_in,
    perms_in,
    mass_ii,
    mass_ib,
    mass_bb,
    psi_in,
    phi_in,
    blocks,
    coupling,
    counts,
    codes,
    perms,
    m_ii,
    m_bb,
    lhs,
    rhs,
    placed,
    near,
    far,
    held,
    key_mine,
    key_got,
    hot,
    sums,
    part,
    passed,
    landed,
    small_sem,
    in_sem,
    send_sem,
    got_sem,
    key_send_sem,
    key_sem,
    pass_send_sem,
    pass_sem,
):
    grp = lax.axis_index("grp")
    me = lax.axis_index("sub")
    slots, interior, width = psi_in.shape
    own_rows = width // n_sub
    half = n_sub // 2
    quad = half // 2
    lanes = n_sub * ROWS
    part_rows = NBG * ROWS
    cut = width // 2
    other = 1 - grp
    spot = lax.rem(me, half)
    first = me - spot
    beyond = half - first
    corner = lax.rem(me, quad)
    member = grp * half + spot
    reach = grp + me // quad + lax.rem(me // 2, 2)
    gate = jnp.maximum(slots - 1 - reach, 0)

    def loads(slot):
        pairs = (
            (psi_in, lhs.at[slot, :, pl.ds(0, width)]),
            (mass_ii, m_ii.at[slot]),
            (mass_ib, rhs.at[slot, :, pl.ds(width, width)]),
            (mass_bb, m_bb.at[slot]),
            (phi_in, lhs.at[slot, :, pl.ds(width, lhs.shape[2] - width)]),
        )
        return [
            pltpu.make_async_copy(source.at[slot], into, in_sem.at[slot, index])
            for index, (source, into) in enumerate(pairs)
        ]

    small = [
        pltpu.make_async_copy(source, into, small_sem.at[index])
        for index, (source, into) in enumerate(
            ((counts_in, counts), (codes_in, codes), (perms_in, perms))
        )
    ]
    for copy in small + loads(0):
        copy.start()
    def peer_at(base, plane, turn, step):
        low = plane * quad + lax.rem(me + step, quad)
        return lax.rem(grp + turn, n_grp), base + low

    steps = [(1, 2), (0, 2), (1, 3), (0, 3), (1, 1), (1, 0), (0, 1), (0, 0)]
    own_plane = spot // quad
    across = [[peer_at(beyond, plane, *step) for step in steps] for plane in range(2)]
    beside = [peer_at(first, own_plane, *step) for step in steps[:-1]]
    stacked = [peer_at(first, 1 - own_plane, *step) for step in steps]
    inner = 1 - me // half
    is_inner = own_plane == inner
    is_outer = own_plane != inner
    inward = [peer_at(first, inner, *step) for step in steps]
    barrier = pltpu.get_barrier_semaphore()

    def greet(peer):
        pl.semaphore_signal(barrier, inc=1, device_id=peer, device_id_type=MESH)

    for peer in across[0] + across[1] + stacked + beside:
        greet(peer)

    def row_of(peer, owner):
        return pl.multiple_of(owner * own_rows + peer[0] * ROWS, ROWS)

    def push(source, into, kind, slot, peer):
        pltpu.make_async_remote_copy(
            src_ref=source,
            dst_ref=into,
            send_sem=send_sem.at[kind, slot],
            recv_sem=got_sem.at[kind, slot],
            device_id=peer,
            device_id_type=MESH,
        ).start()

    def make_keys():
        lane = lax.broadcasted_iota(jnp.int32, (1, lanes), 1)
        for slot in range(slots):
            code = codes[slot]
            block = lax.rem(grp + code // NBG, n_grp) * NBG + lax.rem(code, NBG)
            block = jnp.where(slot < counts[0], block, -n_grp * NBG) * ROWS
            key_mine[slot] = jnp.where(lane // ROWS == member, block + lane % ROWS, 0)
        key_got[0, pl.ds(member, 1)] = key_mine[...][None]

    def send_keys():
        def key_copy(side, peer):
            pltpu.make_async_remote_copy(
                src_ref=key_mine,
                dst_ref=key_got.at[side, member],
                send_sem=key_send_sem.at[side],
                recv_sem=key_sem.at[side],
                device_id=peer,
                device_id_type=MESH,
            ).start()

        for peer in across[0] + across[1]:
            key_copy(1, peer)
        for peer in stacked + beside:
            key_copy(0, peer)

    def send_far(slot):
        for peer in across[1]:
            rows = pl.ds(row_of(peer, peer[1]), ROWS)
            push(placed.at[slot, rows, :], far.at[slot, member], 0, slot, peer)

    def send_held(slot):
        def one(peer):
            owner = beyond + peer[1] - first - inner * quad
            rows = pl.ds(row_of(peer, owner), ROWS)
            push(placed.at[slot, rows, :], held.at[slot, member], 2, slot, peer)

        for peer in inward[:-1]:
            one(peer)
        pl.when(is_outer)(functools.partial(one, inward[-1]))

    def send_near(slot, peers):
        for peer in peers:
            rows = pl.ds(row_of(peer, peer[1]), ROWS)
            push(placed.at[slot, rows, :], near.at[slot, member], 1, slot, peer)

    def spread(slot):
        send_held(slot)
        send_far(slot)
        if slot == 0:
            send_keys()
        send_near(slot, beside)

        @pl.when(is_inner)
        def outward():
            send_near(slot, stacked)

        if slot == slots - 1:

            @pl.when(is_outer)
            def last():
                for late in range(slots):
                    send_near(late, stacked)

    def reduce_slot(slot):
        for copy in loads(slot) + (small if slot == 0 else []):
            copy.wait()
        if slot + 1 < slots:
            for copy in loads(slot + 1):
                copy.start()
        modes = lhs[slot, :, :width]
        step = interior // STRIPS
        for top in range(0, interior, step):
            made = dot(m_ii[slot, top : top + step, :], modes).astype(jnp.bfloat16)
            rhs[slot, top : top + step, :width] = made
        if slot > 0:

            @pl.when(gate == slot)
            def enter():
                pl.semaphore_wait(barrier, 2 * n_sub - 1)
                for early in range(slot):
                    spread(early)

        every = dot(lhs[slot], rhs[slot], 0, 0)
        cross = every[:width, width:]
        direct = every[:width, :width] + cross + m_bb[slot].astype(jnp.float32)
        place = lax.broadcasted_iota(jnp.int32, (width, width), 0)
        pick = jnp.where(place == perms[pl.ds(slot, 1), :], 1.0, 0.0).astype(jnp.bfloat16)
        high, low = split(direct)
        cross_high, cross_low = split(cross)
        rows = dot(pick, high) + dot(pick, low)
        rows = rows + dot(pick, cross_high, 1, 1) + dot(pick, cross_low, 1, 1)
        high, low = split(rows)
        placed[slot] = dot(high, pick, 1, 1) + dot(low, pick, 1, 1)
        active = jnp.where(slot < counts[0], 1.0, 0.0)
        coupling[slot] = (every[width:, :width] + every[width:, width:]) * active
        mine = pl.ds(row_of((grp, me), me), ROWS)
        near[slot, pl.ds(member, 1)] = placed[slot, mine, :][None]
        mine = pl.ds(row_of((grp, me), beyond + corner), ROWS)
        held[slot, pl.ds(member, 1)] = placed[slot, mine, :][None]

    for slot in range(slots):
        reduce_slot(slot)
        if slot == 0:
            make_keys()

        if slot == 0:

            @pl.when(gate == slot)
            def enter():
                pl.semaphore_wait(barrier, 2 * n_sub - 1)

        @pl.when(gate <= slot)
        def follow():
            spread(slot)


    many = n_sub - 1

    def settle(ref, sem):
        pltpu.make_async_copy(ref, ref, sem).wait()

    settle(key_got.at[0, pl.ds(0, many)], key_sem.at[0])
    settle(key_got.at[1], key_sem.at[1])
    target = lax.broadcasted_iota(jnp.int32, (n_grp * part_rows, lanes), 0)
    for side in range(2):
        keys = jnp.sum(key_got[side], axis=0)
        for slot in range(slots):
            hot[side, slot] = jnp.where(target == keys[slot], 1.0, 0.0).astype(jnp.bfloat16)

    def gather(side, slot, got):
        high, low = split(got.reshape(lanes, got.shape[-1]))
        return dot(hot[side, slot], high) + dot(hot[side, slot], low)

    def hand(to):
        return pltpu.make_async_remote_copy(
            src_ref=part.at[pl.ds(pl.multiple_of(to * part_rows, part_rows), part_rows)],
            dst_ref=landed.at[grp],
            send_sem=pass_send_sem.at[0],
            recv_sem=pass_sem.at[grp],
            device_id=(to, beyond + corner),
            device_id_type=MESH,
        )

    @pl.when(is_inner)
    def fold():
        total = None
        for slot in range(slots):
            settle(held.at[slot, pl.ds(0, many)], got_sem.at[2, slot])
            one = gather(0, slot, held[slot])
            total = one if total is None else total + one
        part[...] = total
        hand(other).start()
        hand(grp).start()

    def swap(side):
        rows = pl.ds(pl.multiple_of(other * part_rows, part_rows), part_rows)
        return pltpu.make_async_remote_copy(
            src_ref=sums.at[side, rows],
            dst_ref=passed.at[side],
            send_sem=pass_send_sem.at[1 + side],
            recv_sem=pass_sem.at[n_grp + side],
            device_id=(other, me),
            device_id_type=MESH,
        )

    total = None
    for slot in range(slots):
        settle(near.at[slot, pl.ds(0, many)], got_sem.at[1, slot])
        one = gather(0, slot, near[slot])
        total = one if total is None else total + one
    for side in range(2):
        sums[side] = total[:, side * cut : (side + 1) * cut]

    @pl.when(own_plane == 1)
    def direct():
        total = None
        for slot in range(slots):
            settle(far.at[slot], got_sem.at[0, slot])
            one = gather(1, slot, far[slot])
            total = one if total is None else total + one
        for side in range(2):
            sums[side] = sums[side] + total[:, side * cut : (side + 1) * cut]

    for side in range(2):
        swap(side).start()

    settle(key_got.at[0, pl.ds(0, many)], key_send_sem.at[0])
    settle(key_got.at[1], key_send_sem.at[1])
    for slot in range(slots):
        settle(far.at[slot, pl.ds(0, len(steps))], send_sem.at[0, slot])
        settle(near.at[slot, pl.ds(0, many)], send_sem.at[1, slot])
        settle(held.at[slot, pl.ds(0, len(steps) - 1)], send_sem.at[2, slot])

    @pl.when(is_outer)
    def sent():
        for slot in range(slots):
            settle(held.at[slot, pl.ds(0, 1)], send_sem.at[2, slot])

    mine = pl.ds(pl.multiple_of(grp * part_rows, part_rows), part_rows)
    def put(row, side, value):
        into = pl.ds(pl.multiple_of(row * ROWS, ROWS), ROWS)
        blocks[:, into, side * cut : (side + 1) * cut] = value.reshape(NBG, ROWS, cut)

    @pl.when(own_plane == 1)
    def finish():
        for side in range(2):
            put(grp, side, sums[side, mine, :])
        for side in range(2):
            swap(side).wait()
            put(other, side, passed[side])

    @pl.when(own_plane == 0)
    def finish_landed():
        for side in range(2):
            swap(side).wait()
        for place in range(n_grp):
            settle(landed.at[place], pass_sem.at[place])
        for side in range(2):
            columns = slice(side * cut, (side + 1) * cut)
            put(grp, side, sums[side, mine, :] + landed[grp][:, columns])
            put(other, side, passed[side] + landed[other][:, columns])

    @pl.when(is_inner)
    def handed():
        settle(part, pass_send_sem.at[0])


def cross_scratch(n_grp, n_sub, slots, interior, width, modes):
    bf16, f32, i32 = jnp.bfloat16, jnp.float32, jnp.int32
    dma = pltpu.SemaphoreType.DMA
    lanes, cut = n_sub * ROWS, width // 2
    total = n_grp * NBG * ROWS
    return [
        pltpu.SMEM((1,), i32),
        pltpu.SMEM((slots,), i32),
        pltpu.VMEM((slots, width), i32),
        pltpu.VMEM((slots, interior, interior), bf16),
        pltpu.VMEM((slots, width, width), bf16),
        pltpu.VMEM((slots, interior, width + modes), bf16),
        pltpu.VMEM((slots, interior, 2 * width), bf16),
        pltpu.VMEM((slots, width, width), f32),
        pltpu.VMEM((slots, n_sub, ROWS, width), f32),
        pltpu.VMEM((slots, n_sub, ROWS, width), f32),
        pltpu.VMEM((slots, n_sub, ROWS, width), f32),
        pltpu.VMEM((slots, 1, lanes), i32),
        pltpu.VMEM((2, n_sub, slots, 1, lanes), i32),
        pltpu.VMEM((2, slots, total, lanes), bf16),
        pltpu.VMEM((2, total, cut), f32),
        pltpu.VMEM((total, width), f32),
        pltpu.VMEM((2, NBG * ROWS, cut), f32),
        pltpu.VMEM((n_grp, NBG * ROWS, width), f32),
        dma((3,)),
        dma((slots, 5)),
        dma((3, slots)),
        dma((3, slots)),
        dma((2,)),
        dma((2,)),
        dma((3,)),
        dma((n_grp + 2,)),
    ]


def per_device(n_grp, n_sub, counts, block_map, perms, mass_ii, mass_ib, mass_bb, psi, phi):
    slots, interior, width = psi.shape
    modes = phi.shape[2]
    own_rows = width // n_sub
    chunks = own_rows // ROWS * (width // LANES)
    lanes = n_sub * ROWS
    body = kernel
    fits = n_grp == 2 and n_sub * ROWS == LANES and own_rows == 2 * ROWS and width == 2 * LANES
    key_rows = -(-slots // 8) * 8
    smem = pl.BlockSpec(memory_space=pltpu.SMEM)
    vmem = pl.BlockSpec(memory_space=pltpu.VMEM)
    hbm = pl.BlockSpec(memory_space=pl.ANY)
    vmem_in = vmem
    bf16, f32, i32 = jnp.bfloat16, jnp.float32, jnp.int32
    dma = pltpu.SemaphoreType.DMA
    scratch = [
        pltpu.VMEM(mass_ii.shape, bf16),
        pltpu.VMEM(mass_bb.shape, bf16),
        pltpu.VMEM((slots, interior, width + modes), bf16),
        pltpu.VMEM((slots, interior, 2 * width), bf16),
        pltpu.VMEM((slots, width, width), f32),
        pltpu.VMEM((chunks, slots, n_sub, ROWS, LANES), f32),
        pltpu.VMEM((key_rows, lanes), i32),
        pltpu.VMEM((n_sub, key_rows, lanes), i32),
        pltpu.VMEM((slots, 2 * NBG * ROWS, lanes), bf16),
        pltpu.VMEM((chunks, 2 * NBG * ROWS, LANES), f32),
        pltpu.VMEM((chunks, NBG * ROWS, LANES), f32),
        dma((slots, 5)),
        dma((chunks, slots)),
        dma((chunks, slots)),
        dma,
        dma,
        dma((chunks,)),
        dma((chunks,)),
    ]
    if fits and interior % STRIPS == 0:
        body, smem, vmem_in = cross_kernel, hbm, hbm
        scratch = cross_scratch(n_grp, n_sub, slots, interior, width, modes)
    return pl.pallas_call(
        functools.partial(body, n_grp, n_sub),
        out_shape=(
            pltpu.VMEM((NBG, own_rows, width), f32),
            pltpu.VMEM((slots, modes, width), f32),
        ),
        in_specs=[smem, smem, vmem_in] + [hbm] * 5,
        out_specs=(vmem, vmem),
        scratch_shapes=scratch,
        compiler_params=pltpu.CompilerParams(
            collective_id=0, has_side_effects=True, vmem_limit_bytes=56 * 1024 * 1024
        ),
    )(counts, block_map, perms, mass_ii, mass_ib, mass_bb, psi, phi)


def solution(mesh):
    both = P(("grp", "sub"))
    return jax.shard_map(
        functools.partial(per_device, mesh.shape["grp"], mesh.shape["sub"]),
        mesh=mesh,
        in_specs=(both,) * 8,
        out_specs=(P("grp", "sub", None), both),
        check_vma=False,
    )
```

```python
import functools

import jax
import jax.numpy as jnp
from jax import lax
from jax.experimental import pallas as pl
from jax.experimental.pallas import tpu as pltpu
from jax.sharding import PartitionSpec as P

NBG = 16
ROWS = 8
LANES = 128
WINDOW = 2
STRIPS = 4
MESH = pl.DeviceIdType.MESH


def split(value):
    high = value.astype(jnp.bfloat16)
    low = (value - high.astype(jnp.float32)).astype(jnp.bfloat16)
    return high, low


def dot(left, right, left_dim=1, right_dim=0):
    return lax.dot_general(
        left,
        right,
        (((left_dim,), (right_dim,)), ((), ())),
        preferred_element_type=jnp.float32,
    )


def send_order(peers):
    return sorted(range(1, peers), key=lambda step: (abs(step - peers // 2), step))


def kernel(
    n_grp,
    n_sub,
    counts,
    codes,
    perms,
    mass_ii,
    mass_ib,
    mass_bb,
    psi_in,
    phi_in,
    blocks,
    coupling,
    m_ii,
    m_bb,
    lhs,
    rhs,
    placed,
    got,
    key_mine,
    key_got,
    hot,
    sums,
    passed,
    in_sem,
    send_sem,
    got_sem,
    key_send_sem,
    key_sem,
    pass_send_sem,
    pass_sem,
):
    grp = lax.axis_index("grp")
    me = lax.axis_index("sub")
    slots, interior, width = psi_in.shape
    chunks = got.shape[0]
    cuts = width // LANES
    own_rows = chunks // cuts * ROWS
    lanes = n_sub * ROWS
    after = lax.rem(grp + 1, n_grp)
    before = lax.rem(grp + n_grp - 1, n_grp)

    def loads(slot):
        pairs = (
            (psi_in, lhs.at[slot, :, pl.ds(0, width)]),
            (mass_ii, m_ii.at[slot]),
            (mass_ib, rhs.at[slot, :, pl.ds(width, width)]),
            (mass_bb, m_bb.at[slot]),
            (phi_in, lhs.at[slot, :, pl.ds(width, lhs.shape[2] - width)]),
        )
        return [
            pltpu.make_async_copy(source.at[slot], held, in_sem.at[slot, index])
            for index, (source, held) in enumerate(pairs)
        ]

    for copy in loads(0):
        copy.start()

    order = send_order(n_sub)
    peers = [lax.rem(me + step, n_sub) for step in order]
    barrier = pltpu.get_barrier_semaphore()
    for peer in peers:
        pl.semaphore_signal(barrier, inc=1, device_id=(grp, peer), device_id_type=MESH)
    pl.semaphore_signal(barrier, inc=1, device_id=(after, me), device_id_type=MESH)
    greeted = len(peers) + 1
    if n_grp > 2:
        pl.semaphore_signal(barrier, inc=1, device_id=(before, me), device_id_type=MESH)
        greeted += 1

    lane = lax.broadcasted_iota(jnp.int32, (1, lanes), 1)
    key_mine[...] = jnp.zeros_like(key_mine)
    for slot in range(slots):
        code = jnp.where(slot < counts[0], codes[slot] * ROWS, -2 * NBG * ROWS)
        key_mine[slot : slot + 1, :] = jnp.where(lane // ROWS == me, code + lane % ROWS, 0)
    key_got[pl.ds(me, 1)] = key_mine[...][None]

    def key_copy(peer):
        return pltpu.make_async_remote_copy(
            src_ref=key_mine,
            dst_ref=key_got.at[me],
            send_sem=key_send_sem,
            recv_sem=key_sem,
            device_id=(grp, peer),
            device_id_type=MESH,
        )

    def send(chunk, slot):
        for peer in peers:
            top = pl.multiple_of(peer * own_rows + chunk // cuts * ROWS, ROWS)
            left = chunk % cuts * LANES
            pltpu.make_async_remote_copy(
                src_ref=placed.at[slot, pl.ds(top, ROWS), pl.ds(left, LANES)],
                dst_ref=got.at[chunk, slot, me],
                send_sem=send_sem.at[chunk, slot],
                recv_sem=got_sem.at[chunk, slot],
                device_id=(grp, peer),
                device_id_type=MESH,
            ).start()

    @pl.loop(0, slots)
    def one_slot(slot):
        copies = loads(slot)

        @pl.when(slot + 1 < slots)
        def ahead_loads():
            for copy in loads(slot + 1):
                copy.start()

        copies[0].wait()
        copies[1].wait()
        step = min(interior, 256)
        modes = lhs[slot, :, :width]
        for top in range(0, interior, step):
            made = dot(m_ii[slot, top : top + step, :], modes).astype(jnp.bfloat16)
            rhs[slot, top : top + step, :width] = made
        for copy in copies[2:]:
            copy.wait()
        every = dot(lhs[slot], rhs[slot], 0, 0)
        cross = every[:width, width:]
        direct = every[:width, :width] + cross + m_bb[slot].astype(jnp.float32)
        place = lax.broadcasted_iota(jnp.int32, (width, width), 0)
        pick = jnp.where(place == perms[pl.ds(slot, 1), :], 1.0, 0.0).astype(jnp.bfloat16)
        high, low = split(direct)
        cross_high, cross_low = split(cross)
        rows = dot(pick, high) + dot(pick, low)
        rows = rows + dot(pick, cross_high, 1, 1) + dot(pick, cross_low, 1, 1)
        high, low = split(rows)
        placed[slot] = dot(high, pick, 1, 1) + dot(low, pick, 1, 1)
        active = jnp.where(slot < counts[0], 1.0, 0.0)
        coupling[slot] = (every[width:, :width] + every[width:, width:]) * active
        for chunk in range(chunks):
            mine = pl.multiple_of(me * own_rows + chunk // cuts * ROWS, ROWS)
            left = chunk % cuts * LANES
            own = placed[slot, pl.ds(mine, ROWS), left : left + LANES]
            got[chunk, slot, pl.ds(me, 1)] = own[None]

        @pl.when(slot == 0)
        def enter():
            pl.semaphore_wait(barrier, greeted)
            for peer in peers:
                key_copy(peer).start()

        @pl.when(slot < slots - 1)
        def spread():
            for chunk in range(chunks):
                send(chunk, slot)

    window = min(WINDOW, chunks)
    for chunk in range(window):
        send(chunk, slots - 1)

    many = n_sub - 1
    all_keys = key_got.at[pl.ds(0, many)]
    pltpu.make_async_copy(all_keys, all_keys, key_sem).wait()
    keys = jnp.sum(key_got[...], axis=0)
    target = lax.broadcasted_iota(jnp.int32, (2 * NBG * ROWS, lanes), 0)
    for slot in range(slots):
        hot[slot] = jnp.where(target == keys[slot : slot + 1, :], 1.0, 0.0).astype(jnp.bfloat16)

    def pass_copy(chunk):
        return pltpu.make_async_remote_copy(
            src_ref=sums.at[chunk, pl.ds(NBG * ROWS, NBG * ROWS)],
            dst_ref=passed.at[chunk],
            send_sem=pass_send_sem.at[chunk],
            recv_sem=pass_sem.at[chunk],
            device_id=(after, me),
            device_id_type=MESH,
        )

    def owner_sum(chunk, slot):
        arrived = got.at[chunk, slot, pl.ds(0, many)]
        pltpu.make_async_copy(arrived, arrived, got_sem.at[chunk, slot]).wait()
        high, low = split(got[chunk, slot].reshape(lanes, LANES))
        return dot(hot[slot], high) + dot(hot[slot], low)

    for slot in range(slots):
        for chunk in range(chunks):
            total = owner_sum(chunk, slot)
            if slot > 0:
                total = total + sums[chunk]
            sums[chunk] = total
            if slot == slots - 1:
                pass_copy(chunk).start()
                if chunk + window < chunks:
                    send(chunk + window, slot)

    for chunk in range(chunks):
        pass_copy(chunk).wait()
        own = sums[chunk, : NBG * ROWS] + passed[chunk]
        top, left = chunk // cuts * ROWS, chunk % cuts * LANES
        blocks[:, top : top + ROWS, left : left + LANES] = own.reshape(NBG, ROWS, LANES)

    pltpu.make_async_copy(all_keys, all_keys, key_send_sem).wait()
    for chunk in range(chunks):
        for slot in range(slots):
            arrived = got.at[chunk, slot, pl.ds(0, many)]
            pltpu.make_async_copy(arrived, arrived, send_sem.at[chunk, slot]).wait()


def cross_kernel(
    n_grp,
    n_sub,
    counts_in,
    codes_in,
    perms_in,
    mass_ii,
    mass_ib,
    mass_bb,
    psi_in,
    phi_in,
    blocks,
    coupling,
    counts,
    codes,
    perms,
    m_ii,
    m_bb,
    lhs,
    rhs,
    placed,
    near,
    far,
    held,
    key_mine,
    key_got,
    hot,
    sums,
    part,
    passed,
    landed,
    small_sem,
    in_sem,
    send_sem,
    got_sem,
    key_send_sem,
    key_sem,
    pass_send_sem,
    pass_sem,
):
    grp = lax.axis_index("grp")
    me = lax.axis_index("sub")
    slots, interior, width = psi_in.shape
    own_rows = width // n_sub
    half = n_sub // 2
    quad = half // 2
    lanes = n_sub * ROWS
    part_rows = NBG * ROWS
    cut = width // 2
    other = 1 - grp
    spot = lax.rem(me, half)
    first = me - spot
    beyond = half - first
    corner = lax.rem(me, quad)
    member = grp * half + spot
    reach = grp + me // quad + lax.rem(me // 2, 2)
    gate = jnp.maximum(slots - 1 - reach, 0)

    def loads(slot):
        pairs = (
            (psi_in, lhs.at[slot, :, pl.ds(0, width)]),
            (mass_ii, m_ii.at[slot]),
            (mass_ib, rhs.at[slot, :, pl.ds(width, width)]),
            (mass_bb, m_bb.at[slot]),
            (phi_in, lhs.at[slot, :, pl.ds(width, lhs.shape[2] - width)]),
        )
        return [
            pltpu.make_async_copy(source.at[slot], into, in_sem.at[slot, index])
            for index, (source, into) in enumerate(pairs)
        ]

    small = [
        pltpu.make_async_copy(source, into, small_sem.at[index])
        for index, (source, into) in enumerate(
            ((counts_in, counts), (codes_in, codes), (perms_in, perms))
        )
    ]
    for copy in small + loads(0):
        copy.start()
    def peer_at(base, plane, turn, step):
        low = plane * quad + lax.rem(me + step, quad)
        return lax.rem(grp + turn, n_grp), base + low

    steps = [(1, 2), (0, 2), (1, 3), (0, 3), (1, 1), (1, 0), (0, 1), (0, 0)]
    own_plane = spot // quad
    across = [[peer_at(beyond, plane, *step) for step in steps] for plane in range(2)]
    beside = [peer_at(first, own_plane, *step) for step in steps[:-1]]
    stacked = [peer_at(first, 1 - own_plane, *step) for step in steps]
    inner = 1 - me // half
    is_inner = own_plane == inner
    is_outer = own_plane != inner
    prompt = own_plane + first > 0
    inward = [peer_at(first, inner, *step) for step in steps]
    barrier = pltpu.get_barrier_semaphore()

    def greet(peer):
        pl.semaphore_signal(barrier, inc=1, device_id=peer, device_id_type=MESH)

    for peer in across[0] + across[1] + stacked + beside:
        greet(peer)

    def row_of(peer, owner):
        return pl.multiple_of(owner * own_rows + peer[0] * ROWS, ROWS)

    def push(source, into, kind, slot, peer):
        pltpu.make_async_remote_copy(
            src_ref=source,
            dst_ref=into,
            send_sem=send_sem.at[kind, slot],
            recv_sem=got_sem.at[kind, slot],
            device_id=peer,
            device_id_type=MESH,
        ).start()

    def make_keys():
        lane = lax.broadcasted_iota(jnp.int32, (1, lanes), 1)
        row = jnp.zeros((1, lanes), jnp.int32)
        for slot in range(slots):
            code = codes[slot]
            block = lax.rem(grp + code // NBG, n_grp) * NBG + lax.rem(code, NBG)
            block = jnp.where(slot < counts[0], block, -n_grp * NBG)
            row = row + jnp.where(lane == member * ROWS + slot, block, 0)
        key_mine[...] = row
        key_got[0, pl.ds(member, 1)] = row[None]

    def send_keys():
        def key_copy(side, peer):
            pltpu.make_async_remote_copy(
                src_ref=key_mine,
                dst_ref=key_got.at[side, member],
                send_sem=key_send_sem.at[side],
                recv_sem=key_sem.at[side],
                device_id=peer,
                device_id_type=MESH,
            ).start()

        for peer in across[0] + across[1]:
            key_copy(1, peer)
        for peer in stacked + beside:
            key_copy(0, peer)

    def send_far(slot):
        for peer in across[1]:
            rows = pl.ds(row_of(peer, peer[1]), ROWS)
            push(placed.at[slot, rows, :], far.at[slot, member], 0, slot, peer)

    def send_held(slot):
        def one(peer):
            owner = beyond + peer[1] - first - inner * quad
            rows = pl.ds(row_of(peer, owner), ROWS)
            push(placed.at[slot, rows, :], held.at[slot, member], 2, slot, peer)

        for peer in inward[:-1]:
            one(peer)
        pl.when(is_outer)(functools.partial(one, inward[-1]))

    def send_near(slot, side, peers):
        for peer in peers:
            rows = pl.ds(row_of(peer, peer[1]), ROWS)
            source = placed.at[slot, rows, pl.ds(side * cut, cut)]
            push(source, near.at[side, slot, member], 1 + 2 * side, slot, peer)

    def spread(slot):
        send_held(slot)

        @pl.when(prompt)
        def at_once():
            send_far(slot)

        if slot > 0:

            @pl.when(jnp.logical_not(prompt))
            def one_late():
                send_far(slot - 1)
                if slot == slots - 1:
                    send_far(slot)

        if slot == 0:
            send_keys()
        for side in (1, 0):
            send_near(slot, side, beside)

        @pl.when(is_inner)
        def outward():
            for side in (1, 0):
                send_near(slot, side, stacked)

        if slot == slots - 1:

            @pl.when(is_outer)
            def last():
                for side in (1, 0):
                    for late in range(slots):
                        send_near(late, side, stacked)

    def reduce_slot(slot):
        for copy in loads(slot) + (small if slot == 0 else []):
            copy.wait()
        if slot + 1 < slots:
            for copy in loads(slot + 1):
                copy.start()
        modes = lhs[slot, :, :width]
        step = interior // STRIPS
        for top in range(0, interior, step):
            made = dot(m_ii[slot, top : top + step, :], modes).astype(jnp.bfloat16)
            rhs[slot, top : top + step, :width] = made
        if slot > 0:

            @pl.when(gate == slot)
            def enter():
                pl.semaphore_wait(barrier, 2 * n_sub - 1)
                for early in range(slot):
                    spread(early)

        every = dot(lhs[slot], rhs[slot], 0, 0)
        cross = every[:width, width:]
        direct = every[:width, :width] + cross + m_bb[slot].astype(jnp.float32)
        place = lax.broadcasted_iota(jnp.int32, (width, width), 0)
        pick = jnp.where(place == perms[pl.ds(slot, 1), :], 1.0, 0.0).astype(jnp.bfloat16)
        high, low = split(direct)
        cross_high, cross_low = split(cross)
        rows = dot(pick, high) + dot(pick, low)
        rows = rows + dot(pick, cross_high, 1, 1) + dot(pick, cross_low, 1, 1)
        high, low = split(rows)
        placed[slot] = dot(high, pick, 1, 1) + dot(low, pick, 1, 1)
        active = jnp.where(slot < counts[0], 1.0, 0.0)
        coupling[slot] = (every[width:, :width] + every[width:, width:]) * active
        mine = pl.ds(row_of((grp, me), me), ROWS)
        for side in range(2):
            own = placed[slot, mine, side * cut : (side + 1) * cut]
            near[side, slot, pl.ds(member, 1)] = own[None]
        mine = pl.ds(row_of((grp, me), beyond + corner), ROWS)
        held[slot, pl.ds(member, 1)] = placed[slot, mine, :][None]

    for slot in range(slots):
        reduce_slot(slot)
        if slot == 0:
            make_keys()

        if slot == 0:

            @pl.when(gate == slot)
            def enter():
                pl.semaphore_wait(barrier, 2 * n_sub - 1)

        @pl.when(gate <= slot)
        def follow():
            spread(slot)


    many = n_sub - 1

    def settle(ref, sem):
        pltpu.make_async_copy(ref, ref, sem).wait()

    settle(key_got.at[0, pl.ds(0, many)], key_sem.at[0])
    settle(key_got.at[1], key_sem.at[1])
    target = lax.broadcasted_iota(jnp.int32, (n_grp * part_rows, lanes), 0)
    target = target.astype(jnp.float32)
    source = lax.broadcasted_iota(jnp.int32, (lanes, lanes), 0)
    lane = lax.broadcasted_iota(jnp.int32, (lanes, lanes), 1)
    lead = lane - lane % ROWS
    within = (lane[:1] % ROWS).astype(jnp.float32)
    for side in range(2):
        keys = jnp.sum(key_got[side], axis=0).astype(jnp.float32)
        keys = jnp.broadcast_to(keys, (ROWS, lanes)).astype(jnp.bfloat16)
        for slot in range(slots):
            move = jnp.where(source == lead + slot, 1.0, 0.0).astype(jnp.bfloat16)
            key = dot(keys, move)[:1] * ROWS + within
            hot[side, slot] = jnp.where(target == key, 1.0, 0.0).astype(jnp.bfloat16)

    def gather(side, slot, got):
        high, low = split(got.reshape(lanes, got.shape[-1]))
        return dot(hot[side, slot], high) + dot(hot[side, slot], low)

    def hand(to):
        return pltpu.make_async_remote_copy(
            src_ref=part.at[pl.ds(pl.multiple_of(to * part_rows, part_rows), part_rows)],
            dst_ref=landed.at[grp],
            send_sem=pass_send_sem.at[0],
            recv_sem=pass_sem.at[grp],
            device_id=(to, beyond + corner),
            device_id_type=MESH,
        )

    @pl.when(is_inner)
    def fold():
        total = None
        for slot in range(slots):
            settle(held.at[slot, pl.ds(0, many)], got_sem.at[2, slot])
            one = gather(0, slot, held[slot])
            total = one if total is None else total + one
        part[...] = total
        hand(other).start()
        hand(grp).start()

    def swap(side):
        rows = pl.ds(pl.multiple_of(other * part_rows, part_rows), part_rows)
        return pltpu.make_async_remote_copy(
            src_ref=sums.at[side, rows],
            dst_ref=passed.at[side],
            send_sem=pass_send_sem.at[1 + side],
            recv_sem=pass_sem.at[n_grp + side],
            device_id=(other, me),
            device_id_type=MESH,
        )

    def near_sum(side):
        total = None
        for slot in range(slots):
            settle(near.at[side, slot, pl.ds(0, many)], got_sem.at[1 + 2 * side, slot])
            one = gather(0, slot, near[side, slot])
            total = one if total is None else total + one
        return total

    sums[0] = jnp.zeros_like(sums[0])
    sums[1] = near_sum(1)

    @pl.when(own_plane == 1)
    def direct():
        total = None
        for slot in range(slots):
            settle(far.at[slot], got_sem.at[0, slot])
            one = gather(1, slot, far[slot])
            total = one if total is None else total + one
        sums[1] = sums[1] + total[:, cut:]
        sums[0] = total[:, :cut]

    swap(1).start()
    sums[0] = sums[0] + near_sum(0)
    swap(0).start()

    settle(key_got.at[0, pl.ds(0, many)], key_send_sem.at[0])
    settle(key_got.at[1], key_send_sem.at[1])
    for slot in range(slots):
        settle(far.at[slot, pl.ds(0, len(steps))], send_sem.at[0, slot])
        for side in range(2):
            settle(near.at[side, slot, pl.ds(0, many)], send_sem.at[1 + 2 * side, slot])
        settle(held.at[slot, pl.ds(0, len(steps) - 1)], send_sem.at[2, slot])

    @pl.when(is_outer)
    def sent():
        for slot in range(slots):
            settle(held.at[slot, pl.ds(0, 1)], send_sem.at[2, slot])

    mine = pl.ds(pl.multiple_of(grp * part_rows, part_rows), part_rows)
    def put(row, side, value):
        into = pl.ds(pl.multiple_of(row * ROWS, ROWS), ROWS)
        blocks[:, into, side * cut : (side + 1) * cut] = value.reshape(NBG, ROWS, cut)

    @pl.when(own_plane == 1)
    def finish():
        for side in range(2):
            put(grp, side, sums[side, mine, :])
        for side in (1, 0):
            swap(side).wait()
            put(other, side, passed[side])

    @pl.when(own_plane == 0)
    def finish_landed():
        for place in range(n_grp):
            settle(landed.at[place], pass_sem.at[place])
        for side in (1, 0):
            swap(side).wait()
            columns = slice(side * cut, (side + 1) * cut)
            put(grp, side, sums[side, mine, :] + landed[grp][:, columns])
            put(other, side, passed[side] + landed[other][:, columns])

    @pl.when(is_inner)
    def handed():
        settle(part, pass_send_sem.at[0])


def cross_scratch(n_grp, n_sub, slots, interior, width, modes):
    bf16, f32, i32 = jnp.bfloat16, jnp.float32, jnp.int32
    dma = pltpu.SemaphoreType.DMA
    lanes, cut = n_sub * ROWS, width // 2
    total = n_grp * NBG * ROWS
    return [
        pltpu.SMEM((1,), i32),
        pltpu.SMEM((slots,), i32),
        pltpu.VMEM((slots, width), i32),
        pltpu.VMEM((slots, interior, interior), bf16),
        pltpu.VMEM((slots, width, width), bf16),
        pltpu.VMEM((slots, interior, width + modes), bf16),
        pltpu.VMEM((slots, interior, 2 * width), bf16),
        pltpu.VMEM((slots, width, width), f32),
        pltpu.VMEM((2, slots, n_sub, ROWS, cut), f32),
        pltpu.VMEM((slots, n_sub, ROWS, width), f32),
        pltpu.VMEM((slots, n_sub, ROWS, width), f32),
        pltpu.VMEM((1, lanes), i32),
        pltpu.VMEM((2, n_sub, 1, lanes), i32),
        pltpu.VMEM((2, slots, total, lanes), bf16),
        pltpu.VMEM((2, total, cut), f32),
        pltpu.VMEM((total, width), f32),
        pltpu.VMEM((2, NBG * ROWS, cut), f32),
        pltpu.VMEM((n_grp, NBG * ROWS, width), f32),
        dma((3,)),
        dma((slots, 5)),
        dma((4, slots)),
        dma((4, slots)),
        dma((2,)),
        dma((2,)),
        dma((3,)),
        dma((n_grp + 2,)),
    ]


def per_device(n_grp, n_sub, counts, block_map, perms, mass_ii, mass_ib, mass_bb, psi, phi):
    slots, interior, width = psi.shape
    modes = phi.shape[2]
    own_rows = width // n_sub
    chunks = own_rows // ROWS * (width // LANES)
    lanes = n_sub * ROWS
    body = kernel
    fits = n_grp == 2 and n_sub * ROWS == LANES and own_rows == 2 * ROWS and width == 2 * LANES
    key_rows = -(-slots // 8) * 8
    smem = pl.BlockSpec(memory_space=pltpu.SMEM)
    vmem = pl.BlockSpec(memory_space=pltpu.VMEM)
    hbm = pl.BlockSpec(memory_space=pl.ANY)
    vmem_in = vmem
    bf16, f32, i32 = jnp.bfloat16, jnp.float32, jnp.int32
    dma = pltpu.SemaphoreType.DMA
    scratch = [
        pltpu.VMEM(mass_ii.shape, bf16),
        pltpu.VMEM(mass_bb.shape, bf16),
        pltpu.VMEM((slots, interior, width + modes), bf16),
        pltpu.VMEM((slots, interior, 2 * width), bf16),
        pltpu.VMEM((slots, width, width), f32),
        pltpu.VMEM((chunks, slots, n_sub, ROWS, LANES), f32),
        pltpu.VMEM((key_rows, lanes), i32),
        pltpu.VMEM((n_sub, key_rows, lanes), i32),
        pltpu.VMEM((slots, 2 * NBG * ROWS, lanes), bf16),
        pltpu.VMEM((chunks, 2 * NBG * ROWS, LANES), f32),
        pltpu.VMEM((chunks, NBG * ROWS, LANES), f32),
        dma((slots, 5)),
        dma((chunks, slots)),
        dma((chunks, slots)),
        dma,
        dma,
        dma((chunks,)),
        dma((chunks,)),
    ]
    if fits and interior % STRIPS == 0 and slots <= ROWS:
        body, smem, vmem_in = cross_kernel, hbm, hbm
        scratch = cross_scratch(n_grp, n_sub, slots, interior, width, modes)
    return pl.pallas_call(
        functools.partial(body, n_grp, n_sub),
        out_shape=(
            pltpu.VMEM((NBG, own_rows, width), f32),
            pltpu.VMEM((slots, modes, width), f32),
        ),
        in_specs=[smem, smem, vmem_in] + [hbm] * 5,
        out_specs=(vmem, vmem),
        scratch_shapes=scratch,
        compiler_params=pltpu.CompilerParams(
            collective_id=0, has_side_effects=True, vmem_limit_bytes=56 * 1024 * 1024
        ),
    )(counts, block_map, perms, mass_ii, mass_ib, mass_bb, psi, phi)


def solution(mesh):
    both = P(("grp", "sub"))
    return jax.shard_map(
        functools.partial(per_device, mesh.shape["grp"], mesh.shape["sub"]),
        mesh=mesh,
        in_specs=(both,) * 8,
        out_specs=(P("grp", "sub", None), both),
        check_vma=False,
    )
```

```python
import functools

import jax
import jax.numpy as jnp
from jax import lax
from jax.experimental import pallas as pl
from jax.experimental.pallas import tpu as pltpu
from jax.sharding import PartitionSpec as P

NBG = 16
ROWS = 8
LANES = 128
WINDOW = 2
STRIPS = 4
MESH = pl.DeviceIdType.MESH


def split(value):
    high = value.astype(jnp.bfloat16)
    low = (value - high.astype(jnp.float32)).astype(jnp.bfloat16)
    return high, low


def dot(left, right, left_dim=1, right_dim=0):
    return lax.dot_general(
        left,
        right,
        (((left_dim,), (right_dim,)), ((), ())),
        preferred_element_type=jnp.float32,
    )


def send_order(peers):
    return sorted(range(1, peers), key=lambda step: (abs(step - peers // 2), step))


def kernel(
    n_grp,
    n_sub,
    counts,
    codes,
    perms,
    mass_ii,
    mass_ib,
    mass_bb,
    psi_in,
    phi_in,
    blocks,
    coupling,
    m_ii,
    m_bb,
    lhs,
    rhs,
    placed,
    got,
    key_mine,
    key_got,
    hot,
    sums,
    passed,
    in_sem,
    send_sem,
    got_sem,
    key_send_sem,
    key_sem,
    pass_send_sem,
    pass_sem,
):
    grp = lax.axis_index("grp")
    me = lax.axis_index("sub")
    slots, interior, width = psi_in.shape
    chunks = got.shape[0]
    cuts = width // LANES
    own_rows = chunks // cuts * ROWS
    lanes = n_sub * ROWS
    after = lax.rem(grp + 1, n_grp)
    before = lax.rem(grp + n_grp - 1, n_grp)

    def loads(slot):
        pairs = (
            (psi_in, lhs.at[slot, :, pl.ds(0, width)]),
            (mass_ii, m_ii.at[slot]),
            (mass_ib, rhs.at[slot, :, pl.ds(width, width)]),
            (mass_bb, m_bb.at[slot]),
            (phi_in, lhs.at[slot, :, pl.ds(width, lhs.shape[2] - width)]),
        )
        return [
            pltpu.make_async_copy(source.at[slot], held, in_sem.at[slot, index])
            for index, (source, held) in enumerate(pairs)
        ]

    for copy in loads(0):
        copy.start()

    order = send_order(n_sub)
    peers = [lax.rem(me + step, n_sub) for step in order]
    barrier = pltpu.get_barrier_semaphore()
    for peer in peers:
        pl.semaphore_signal(barrier, inc=1, device_id=(grp, peer), device_id_type=MESH)
    pl.semaphore_signal(barrier, inc=1, device_id=(after, me), device_id_type=MESH)
    greeted = len(peers) + 1
    if n_grp > 2:
        pl.semaphore_signal(barrier, inc=1, device_id=(before, me), device_id_type=MESH)
        greeted += 1

    lane = lax.broadcasted_iota(jnp.int32, (1, lanes), 1)
    key_mine[...] = jnp.zeros_like(key_mine)
    for slot in range(slots):
        code = jnp.where(slot < counts[0], codes[slot] * ROWS, -2 * NBG * ROWS)
        key_mine[slot : slot + 1, :] = jnp.where(lane // ROWS == me, code + lane % ROWS, 0)
    key_got[pl.ds(me, 1)] = key_mine[...][None]

    def key_copy(peer):
        return pltpu.make_async_remote_copy(
            src_ref=key_mine,
            dst_ref=key_got.at[me],
            send_sem=key_send_sem,
            recv_sem=key_sem,
            device_id=(grp, peer),
            device_id_type=MESH,
        )

    def send(chunk, slot):
        for peer in peers:
            top = pl.multiple_of(peer * own_rows + chunk // cuts * ROWS, ROWS)
            left = chunk % cuts * LANES
            pltpu.make_async_remote_copy(
                src_ref=placed.at[slot, pl.ds(top, ROWS), pl.ds(left, LANES)],
                dst_ref=got.at[chunk, slot, me],
                send_sem=send_sem.at[chunk, slot],
                recv_sem=got_sem.at[chunk, slot],
                device_id=(grp, peer),
                device_id_type=MESH,
            ).start()

    @pl.loop(0, slots)
    def one_slot(slot):
        copies = loads(slot)

        @pl.when(slot + 1 < slots)
        def ahead_loads():
            for copy in loads(slot + 1):
                copy.start()

        copies[0].wait()
        copies[1].wait()
        step = min(interior, 256)
        modes = lhs[slot, :, :width]
        for top in range(0, interior, step):
            made = dot(m_ii[slot, top : top + step, :], modes).astype(jnp.bfloat16)
            rhs[slot, top : top + step, :width] = made
        for copy in copies[2:]:
            copy.wait()
        every = dot(lhs[slot], rhs[slot], 0, 0)
        cross = every[:width, width:]
        direct = every[:width, :width] + cross + m_bb[slot].astype(jnp.float32)
        place = lax.broadcasted_iota(jnp.int32, (width, width), 0)
        pick = jnp.where(place == perms[pl.ds(slot, 1), :], 1.0, 0.0).astype(jnp.bfloat16)
        high, low = split(direct)
        cross_high, cross_low = split(cross)
        rows = dot(pick, high) + dot(pick, low)
        rows = rows + dot(pick, cross_high, 1, 1) + dot(pick, cross_low, 1, 1)
        high, low = split(rows)
        placed[slot] = dot(high, pick, 1, 1) + dot(low, pick, 1, 1)
        active = jnp.where(slot < counts[0], 1.0, 0.0)
        coupling[slot] = (every[width:, :width] + every[width:, width:]) * active
        for chunk in range(chunks):
            mine = pl.multiple_of(me * own_rows + chunk // cuts * ROWS, ROWS)
            left = chunk % cuts * LANES
            own = placed[slot, pl.ds(mine, ROWS), left : left + LANES]
            got[chunk, slot, pl.ds(me, 1)] = own[None]

        @pl.when(slot == 0)
        def enter():
            pl.semaphore_wait(barrier, greeted)
            for peer in peers:
                key_copy(peer).start()

        @pl.when(slot < slots - 1)
        def spread():
            for chunk in range(chunks):
                send(chunk, slot)

    window = min(WINDOW, chunks)
    for chunk in range(window):
        send(chunk, slots - 1)

    many = n_sub - 1
    all_keys = key_got.at[pl.ds(0, many)]
    pltpu.make_async_copy(all_keys, all_keys, key_sem).wait()
    keys = jnp.sum(key_got[...], axis=0)
    target = lax.broadcasted_iota(jnp.int32, (2 * NBG * ROWS, lanes), 0)
    for slot in range(slots):
        hot[slot] = jnp.where(target == keys[slot : slot + 1, :], 1.0, 0.0).astype(jnp.bfloat16)

    def pass_copy(chunk):
        return pltpu.make_async_remote_copy(
            src_ref=sums.at[chunk, pl.ds(NBG * ROWS, NBG * ROWS)],
            dst_ref=passed.at[chunk],
            send_sem=pass_send_sem.at[chunk],
            recv_sem=pass_sem.at[chunk],
            device_id=(after, me),
            device_id_type=MESH,
        )

    def owner_sum(chunk, slot):
        arrived = got.at[chunk, slot, pl.ds(0, many)]
        pltpu.make_async_copy(arrived, arrived, got_sem.at[chunk, slot]).wait()
        high, low = split(got[chunk, slot].reshape(lanes, LANES))
        return dot(hot[slot], high) + dot(hot[slot], low)

    for slot in range(slots):
        for chunk in range(chunks):
            total = owner_sum(chunk, slot)
            if slot > 0:
                total = total + sums[chunk]
            sums[chunk] = total
            if slot == slots - 1:
                pass_copy(chunk).start()
                if chunk + window < chunks:
                    send(chunk + window, slot)

    for chunk in range(chunks):
        pass_copy(chunk).wait()
        own = sums[chunk, : NBG * ROWS] + passed[chunk]
        top, left = chunk // cuts * ROWS, chunk % cuts * LANES
        blocks[:, top : top + ROWS, left : left + LANES] = own.reshape(NBG, ROWS, LANES)

    pltpu.make_async_copy(all_keys, all_keys, key_send_sem).wait()
    for chunk in range(chunks):
        for slot in range(slots):
            arrived = got.at[chunk, slot, pl.ds(0, many)]
            pltpu.make_async_copy(arrived, arrived, send_sem.at[chunk, slot]).wait()


def cross_kernel(
    n_grp,
    n_sub,
    counts_in,
    codes_in,
    perms_in,
    mass_ii,
    mass_ib,
    mass_bb,
    psi_in,
    phi_in,
    blocks,
    coupling,
    counts,
    codes,
    perms,
    m_ii,
    m_bb,
    lhs,
    rhs,
    placed,
    near,
    far,
    held,
    key_mine,
    key_got,
    hot,
    sums,
    part,
    passed,
    landed,
    small_sem,
    in_sem,
    send_sem,
    got_sem,
    key_send_sem,
    key_sem,
    pass_send_sem,
    pass_sem,
):
    grp = lax.axis_index("grp")
    me = lax.axis_index("sub")
    slots, interior, width = psi_in.shape
    own_rows = width // n_sub
    half = n_sub // 2
    quad = half // 2
    lanes = n_sub * ROWS
    part_rows = NBG * ROWS
    cut = width // 2
    other = 1 - grp
    spot = lax.rem(me, half)
    first = me - spot
    beyond = half - first
    corner = lax.rem(me, quad)
    member = grp * half + spot
    reach = grp + me // quad + lax.rem(me // 2, 2)
    gate = jnp.where(reach < 2, 1, 0)

    def loads(slot):
        pairs = (
            (psi_in, lhs.at[slot, :, pl.ds(0, width)]),
            (mass_ii, m_ii.at[slot]),
            (mass_ib, rhs.at[slot, :, pl.ds(width, width)]),
            (mass_bb, m_bb.at[slot]),
            (phi_in, lhs.at[slot, :, pl.ds(width, lhs.shape[2] - width)]),
        )
        return [
            pltpu.make_async_copy(source.at[slot], into, in_sem.at[slot, index])
            for index, (source, into) in enumerate(pairs)
        ]

    small = [
        pltpu.make_async_copy(source, into, small_sem.at[index])
        for index, (source, into) in enumerate(
            ((counts_in, counts), (codes_in, codes), (perms_in, perms))
        )
    ]
    for copy in small + loads(0):
        copy.start()
    def peer_at(base, plane, turn, step):
        low = plane * quad + lax.rem(me + step, quad)
        return lax.rem(grp + turn, n_grp), base + low

    steps = [(1, 2), (0, 2), (1, 3), (0, 3), (1, 1), (1, 0), (0, 1), (0, 0)]
    own_plane = spot // quad
    across = [[peer_at(beyond, plane, *step) for step in steps] for plane in range(2)]
    beside = [peer_at(first, own_plane, *step) for step in steps[:-1]]
    stacked = [peer_at(first, 1 - own_plane, *step) for step in steps]
    inner = 1 - me // half
    is_inner = own_plane == inner
    is_outer = own_plane != inner
    prompt = own_plane + first > 0
    inward = [peer_at(first, inner, *step) for step in steps]
    barrier = pltpu.get_barrier_semaphore()

    def greet(peer):
        pl.semaphore_signal(barrier, inc=1, device_id=peer, device_id_type=MESH)

    for peer in across[0] + across[1] + stacked + beside:
        greet(peer)

    def row_of(peer, owner):
        return pl.multiple_of(owner * own_rows + peer[0] * ROWS, ROWS)

    def push(source, into, kind, slot, peer):
        pltpu.make_async_remote_copy(
            src_ref=source,
            dst_ref=into,
            send_sem=send_sem.at[kind, slot],
            recv_sem=got_sem.at[kind, slot],
            device_id=peer,
            device_id_type=MESH,
        ).start()

    def make_keys():
        lane = lax.broadcasted_iota(jnp.int32, (1, lanes), 1)
        row = jnp.zeros((1, lanes), jnp.int32)
        for slot in range(slots):
            code = codes[slot]
            block = lax.rem(grp + code // NBG, n_grp) * NBG + lax.rem(code, NBG)
            block = jnp.where(slot < counts[0], block, -n_grp * NBG)
            row = row + jnp.where(lane == member * ROWS + slot, block, 0)
        key_mine[...] = row
        key_got[0, pl.ds(member, 1)] = row[None]

    def send_keys():
        def key_copy(side, peer):
            pltpu.make_async_remote_copy(
                src_ref=key_mine,
                dst_ref=key_got.at[side, member],
                send_sem=key_send_sem.at[side],
                recv_sem=key_sem.at[side],
                device_id=peer,
                device_id_type=MESH,
            ).start()

        for peer in across[0] + across[1]:
            key_copy(1, peer)
        for peer in stacked + beside:
            key_copy(0, peer)

    def send_far(slot):
        for peer in across[1]:
            rows = pl.ds(row_of(peer, peer[1]), ROWS)
            push(placed.at[slot, rows, :], far.at[slot, member], 0, slot, peer)

    def send_held(slot):
        def one(peer):
            owner = beyond + peer[1] - first - inner * quad
            rows = pl.ds(row_of(peer, owner), ROWS)
            push(placed.at[slot, rows, :], held.at[slot, member], 2, slot, peer)

        for peer in inward[:-1]:
            one(peer)
        pl.when(is_outer)(functools.partial(one, inward[-1]))

    def send_near(slot, side, peers):
        for peer in peers:
            rows = pl.ds(row_of(peer, peer[1]), ROWS)
            source = placed.at[slot, rows, pl.ds(side * cut, cut)]
            push(source, near.at[side, slot, member], 1 + 2 * side, slot, peer)

    def spread(slot):
        def run(words):
            for word in words:
                kind, at = word[0], int(word[1])
                if kind == "h":
                    send_held(at)
                if kind == "f":
                    send_far(at)
                if kind == "s":
                    send_near(at % 3, 1 if at < 3 else 0, stacked)
                if kind == "b":
                    send_near(at, 1, beside)
                    send_near(at, 0, beside)
                if kind == "k":
                    send_keys()

        pl.when(is_inner)(functools.partial(run, [['h0', 'f0', 'k0', 's0', 's3', 'b0'], ['h1', 'f1', 's1', 's4', 'b1'], ['h2', 'f2', 's2', 's5', 'b2']][slot]))
        pl.when(own_plane + first == 0)(functools.partial(run, [['h0', 'k0', 'b0'], ['h1', 'f0', 'b1'], ['h2', 'f1', 'f2', 'b2', 's0', 's1', 's2', 's3', 's4', 's5']][slot]))
        pl.when(own_plane * first == half)(functools.partial(run, [['h0', 'f0', 'k0', 'b0'], ['h1', 'f1', 'b1'], ['h2', 'b2', 's0', 's1', 's2', 'f2', 's3', 's4', 's5']][slot]))

    def reduce_slot(slot):
        for copy in loads(slot) + (small if slot == 0 else []):
            copy.wait()
        if slot + 1 < slots:
            for copy in loads(slot + 1):
                copy.start()
        modes = lhs[slot, :, :width]
        step = interior // STRIPS
        for top in range(0, interior, step):
            made = dot(m_ii[slot, top : top + step, :], modes).astype(jnp.bfloat16)
            rhs[slot, top : top + step, :width] = made
        if slot > 0:

            @pl.when(gate == slot)
            def enter():
                pl.semaphore_wait(barrier, 2 * n_sub - 1)
                for early in range(slot):
                    spread(early)

        every = dot(lhs[slot], rhs[slot], 0, 0)
        cross = every[:width, width:]
        direct = every[:width, :width] + cross + m_bb[slot].astype(jnp.float32)
        place = lax.broadcasted_iota(jnp.int32, (width, width), 0)
        pick = jnp.where(place == perms[pl.ds(slot, 1), :], 1.0, 0.0).astype(jnp.bfloat16)
        high, low = split(direct)
        cross_high, cross_low = split(cross)
        rows = dot(pick, high) + dot(pick, low)
        rows = rows + dot(pick, cross_high, 1, 1) + dot(pick, cross_low, 1, 1)
        high, low = split(rows)
        placed[slot] = dot(high, pick, 1, 1) + dot(low, pick, 1, 1)
        active = jnp.where(slot < counts[0], 1.0, 0.0)
        coupling[slot] = (every[width:, :width] + every[width:, width:]) * active
        mine = pl.ds(row_of((grp, me), me), ROWS)
        for side in range(2):
            own = placed[slot, mine, side * cut : (side + 1) * cut]
            near[side, slot, pl.ds(member, 1)] = own[None]
        mine = pl.ds(row_of((grp, me), beyond + corner), ROWS)
        held[slot, pl.ds(member, 1)] = placed[slot, mine, :][None]

    for slot in range(slots):
        reduce_slot(slot)
        if slot == 0:
            make_keys()

        if slot == 0:

            @pl.when(gate == slot)
            def enter():
                pl.semaphore_wait(barrier, 2 * n_sub - 1)

        @pl.when(gate <= slot)
        def follow():
            spread(slot)


    many = n_sub - 1

    def settle(ref, sem):
        pltpu.make_async_copy(ref, ref, sem).wait()

    settle(key_got.at[0, pl.ds(0, many)], key_sem.at[0])
    settle(key_got.at[1], key_sem.at[1])
    target = lax.broadcasted_iota(jnp.int32, (n_grp * part_rows, lanes), 0)
    target = target.astype(jnp.float32)
    source = lax.broadcasted_iota(jnp.int32, (lanes, lanes), 0)
    lane = lax.broadcasted_iota(jnp.int32, (lanes, lanes), 1)
    lead = lane - lane % ROWS
    within = (lane[:1] % ROWS).astype(jnp.float32)
    for side in range(2):
        keys = jnp.sum(key_got[side], axis=0).astype(jnp.float32)
        keys = jnp.broadcast_to(keys, (ROWS, lanes)).astype(jnp.bfloat16)
        for slot in range(slots):
            move = jnp.where(source == lead + slot, 1.0, 0.0).astype(jnp.bfloat16)
            key = dot(keys, move)[:1] * ROWS + within
            hot[side, slot] = jnp.where(target == key, 1.0, 0.0).astype(jnp.bfloat16)

    def gather(side, slot, got):
        high, low = split(got.reshape(lanes, got.shape[-1]))
        return dot(hot[side, slot], high) + dot(hot[side, slot], low)

    def hand(to):
        return pltpu.make_async_remote_copy(
            src_ref=part.at[pl.ds(pl.multiple_of(to * part_rows, part_rows), part_rows)],
            dst_ref=landed.at[grp],
            send_sem=pass_send_sem.at[0],
            recv_sem=pass_sem.at[grp],
            device_id=(to, beyond + corner),
            device_id_type=MESH,
        )

    @pl.when(is_inner)
    def fold():
        total = None
        for slot in range(slots):
            settle(held.at[slot, pl.ds(0, many)], got_sem.at[2, slot])
            one = gather(0, slot, held[slot])
            total = one if total is None else total + one
        part[...] = total
        early = jnp.where(first > 0, 0, other)
        hand(early).start()
        hand(1 - early).start()

    def swap(side):
        rows = pl.ds(pl.multiple_of(other * part_rows, part_rows), part_rows)
        return pltpu.make_async_remote_copy(
            src_ref=sums.at[side, rows],
            dst_ref=passed.at[side],
            send_sem=pass_send_sem.at[1 + side],
            recv_sem=pass_sem.at[n_grp + side],
            device_id=(other, me),
            device_id_type=MESH,
        )

    def near_sum(side):
        total = None
        for slot in range(slots):
            settle(near.at[side, slot, pl.ds(0, many)], got_sem.at[1 + 2 * side, slot])
            one = gather(0, slot, near[side, slot])
            total = one if total is None else total + one
        return total

    sums[0] = jnp.zeros_like(sums[0])
    sums[1] = near_sum(1)

    @pl.when(own_plane == 1)
    def direct():
        total = None
        for slot in range(slots):
            settle(far.at[slot], got_sem.at[0, slot])
            one = gather(1, slot, far[slot])
            total = one if total is None else total + one
        sums[1] = sums[1] + total[:, cut:]
        sums[0] = total[:, :cut]

    swap(1).start()
    sums[0] = sums[0] + near_sum(0)
    swap(0).start()

    settle(key_got.at[0, pl.ds(0, many)], key_send_sem.at[0])
    settle(key_got.at[1], key_send_sem.at[1])
    for slot in range(slots):
        settle(far.at[slot, pl.ds(0, len(steps))], send_sem.at[0, slot])
        for side in range(2):
            settle(near.at[side, slot, pl.ds(0, many)], send_sem.at[1 + 2 * side, slot])
        settle(held.at[slot, pl.ds(0, len(steps) - 1)], send_sem.at[2, slot])

    @pl.when(is_outer)
    def sent():
        for slot in range(slots):
            settle(held.at[slot, pl.ds(0, 1)], send_sem.at[2, slot])

    mine = pl.ds(pl.multiple_of(grp * part_rows, part_rows), part_rows)
    def put(row, side, value):
        into = pl.ds(pl.multiple_of(row * ROWS, ROWS), ROWS)
        blocks[:, into, side * cut : (side + 1) * cut] = value.reshape(NBG, ROWS, cut)

    @pl.when(own_plane == 1)
    def finish():
        for side in range(2):
            put(grp, side, sums[side, mine, :])
        for side in (1, 0):
            swap(side).wait()
            put(other, side, passed[side])

    @pl.when(own_plane == 0)
    def finish_landed():
        for place in range(n_grp):
            settle(landed.at[place], pass_sem.at[place])
        for side in (1, 0):
            swap(side).wait()
            columns = slice(side * cut, (side + 1) * cut)
            put(grp, side, sums[side, mine, :] + landed[grp][:, columns])
            put(other, side, passed[side] + landed[other][:, columns])

    @pl.when(is_inner)
    def handed():
        settle(part, pass_send_sem.at[0])


def cross_scratch(n_grp, n_sub, slots, interior, width, modes):
    bf16, f32, i32 = jnp.bfloat16, jnp.float32, jnp.int32
    dma = pltpu.SemaphoreType.DMA
    lanes, cut = n_sub * ROWS, width // 2
    total = n_grp * NBG * ROWS
    return [
        pltpu.SMEM((1,), i32),
        pltpu.SMEM((slots,), i32),
        pltpu.VMEM((slots, width), i32),
        pltpu.VMEM((slots, interior, interior), bf16),
        pltpu.VMEM((slots, width, width), bf16),
        pltpu.VMEM((slots, interior, width + modes), bf16),
        pltpu.VMEM((slots, interior, 2 * width), bf16),
        pltpu.VMEM((slots, width, width), f32),
        pltpu.VMEM((2, slots, n_sub, ROWS, cut), f32),
        pltpu.VMEM((slots, n_sub, ROWS, width), f32),
        pltpu.VMEM((slots, n_sub, ROWS, width), f32),
        pltpu.VMEM((1, lanes), i32),
        pltpu.VMEM((2, n_sub, 1, lanes), i32),
        pltpu.VMEM((2, slots, total, lanes), bf16),
        pltpu.VMEM((2, total, cut), f32),
        pltpu.VMEM((total, width), f32),
        pltpu.VMEM((2, NBG * ROWS, cut), f32),
        pltpu.VMEM((n_grp, NBG * ROWS, width), f32),
        dma((3,)),
        dma((slots, 5)),
        dma((4, slots)),
        dma((4, slots)),
        dma((2,)),
        dma((2,)),
        dma((3,)),
        dma((n_grp + 2,)),
    ]


def per_device(n_grp, n_sub, counts, block_map, perms, mass_ii, mass_ib, mass_bb, psi, phi):
    slots, interior, width = psi.shape
    modes = phi.shape[2]
    own_rows = width // n_sub
    chunks = own_rows // ROWS * (width // LANES)
    lanes = n_sub * ROWS
    body = kernel
    fits = n_grp == 2 and n_sub * ROWS == LANES and own_rows == 2 * ROWS and width == 2 * LANES
    key_rows = -(-slots // 8) * 8
    smem = pl.BlockSpec(memory_space=pltpu.SMEM)
    vmem = pl.BlockSpec(memory_space=pltpu.VMEM)
    hbm = pl.BlockSpec(memory_space=pl.ANY)
    vmem_in = vmem
    bf16, f32, i32 = jnp.bfloat16, jnp.float32, jnp.int32
    dma = pltpu.SemaphoreType.DMA
    scratch = [
        pltpu.VMEM(mass_ii.shape, bf16),
        pltpu.VMEM(mass_bb.shape, bf16),
        pltpu.VMEM((slots, interior, width + modes), bf16),
        pltpu.VMEM((slots, interior, 2 * width), bf16),
        pltpu.VMEM((slots, width, width), f32),
        pltpu.VMEM((chunks, slots, n_sub, ROWS, LANES), f32),
        pltpu.VMEM((key_rows, lanes), i32),
        pltpu.VMEM((n_sub, key_rows, lanes), i32),
        pltpu.VMEM((slots, 2 * NBG * ROWS, lanes), bf16),
        pltpu.VMEM((chunks, 2 * NBG * ROWS, LANES), f32),
        pltpu.VMEM((chunks, NBG * ROWS, LANES), f32),
        dma((slots, 5)),
        dma((chunks, slots)),
        dma((chunks, slots)),
        dma,
        dma,
        dma((chunks,)),
        dma((chunks,)),
    ]
    if fits and interior % STRIPS == 0 and slots == 3:
        body, smem, vmem_in = cross_kernel, hbm, hbm
        scratch = cross_scratch(n_grp, n_sub, slots, interior, width, modes)
    return pl.pallas_call(
        functools.partial(body, n_grp, n_sub),
        out_shape=(
            pltpu.VMEM((NBG, own_rows, width), f32),
            pltpu.VMEM((slots, modes, width), f32),
        ),
        in_specs=[smem, smem, vmem_in] + [hbm] * 5,
        out_specs=(vmem, vmem),
        scratch_shapes=scratch,
        compiler_params=pltpu.CompilerParams(
            collective_id=0, has_side_effects=True, vmem_limit_bytes=56 * 1024 * 1024
        ),
    )(counts, block_map, perms, mass_ii, mass_ib, mass_bb, psi, phi)


def solution(mesh):
    both = P(("grp", "sub"))
    return jax.shard_map(
        functools.partial(per_device, mesh.shape["grp"], mesh.shape["sub"]),
        mesh=mesh,
        in_specs=(both,) * 8,
        out_specs=(P("grp", "sub", None), both),
        check_vma=False,
    )
```
